8 devices in a mesh: rep: 1 (over z), r: 2 (over y), s: 4 (over x, core).
Axes of the slice: x: 2, y: 2, z: 1, core: 2. Of those that a mesh axis runs over, the one named last changes fastest.
Arguments:
- x: bfloat16 [8, 4096, 1024], P(('rep', 'r', 's'))
- dy: bfloat16 [8, 4096, 1024], P(('rep', 'r', 's'))
- w_gate: bfloat16 [2, 1024, 2816], P(None, 's')
- w_up: bfloat16 [2, 1024, 2816], P(None, 's')
- w_down: bfloat16 [2, 2816, 1024], P(None, 's')
- m_w_gate: float32 [2, 1024, 2816], P(None, 's')
- m_w_up: float32 [2, 1024, 2816], P(None, 's')
- m_w_down: float32 [2, 2816, 1024], P(None, 's')
- v_w_gate: float32 [2, 1024, 2816], P(None, 's')
- v_w_up: float32 [2, 1024, 2816], P(None, 's')
- v_w_down: float32 [2, 2816, 1024], P(None, 's')
Outputs:
- output 1: bfloat16 [2, 1024, 2816], P('rep', 's')
- output 2: bfloat16 [2, 1024, 2816], P('rep', 's')
- output 3: bfloat16 [2, 2816, 1024], P('rep', 's')
- output 4: float32 [2, 1024, 2816], P('rep', 's')
- output 5: float32 [2, 1024, 2816], P('rep', 's')
- output 6: float32 [2, 2816, 1024], P('rep', 's')
- output 7: float32 [2, 1024, 2816], P('rep', 's')
- output 8: float32 [2, 1024, 2816], P('rep', 's')
- output 9: float32 [2, 2816, 1024], P('rep', 's')
All inputs are finite; a program needn't handle non-finite values.
Results may differ from the reference program's by a relative error of at most 0.022.
Values are sent between devices in bfloat16 or wider.
A program may use at most 2 GiB of HBM per device.

```python
import jax
import jax.numpy as jnp
from jax import lax

SEQUENCES = 8
TOKENS = 4096
D = 1024
FF = 2816
LAYERS = 2
NAMES = ("w_gate", "w_up", "w_down")
SHAPES = {"w_gate": (LAYERS, D, FF), "w_up": (LAYERS, D, FF), "w_down": (LAYERS, FF, D)}


def bump(key, n, height):
    away = (jnp.arange(n, dtype=jnp.int32) - jax.random.randint(key, (), 0, n, jnp.int32)) % n
    return jnp.where(away < n // 8, height, 1.0)


def together(key, own, strength):
    shared = jax.random.normal(key, own.shape[1:], jnp.float32)
    return (own + strength * shared) * lax.rsqrt(1 + strength * strength)


def setup_inputs(seed: int = 0, part: int = 0) -> dict:
    kx, kdy, ka, kb, kz, kf, kh, kl, *keys = jax.random.split(jax.random.key(seed), 8 + 3 * len(NAMES))
    kx, kdy, ka, kb = (jax.random.fold_in(k, part) for k in (kx, kdy, ka, kb))
    kw, km, kv = (keys[i::3] for i in range(3))
    shape = (SEQUENCES, TOKENS, D)
    much_x, much_dy = jax.random.uniform(kz, (2,), jnp.float32, 0.0, 1.0)
    loud = 2.0 ** jax.random.uniform(jax.random.fold_in(kz, 1), (), jnp.float32, -1.0, 2.0)
    layers = 2.0 ** jax.random.uniform(kl, (LAYERS, 1, 1), jnp.float32, -1.0, 1.0)
    x = together(ka, jax.random.normal(kx, shape, jnp.float32), much_x) * bump(kf, D, 4.0)
    dy = together(kb, jax.random.normal(kdy, shape, jnp.float32), much_dy)
    drawn = {"x": x.astype(jnp.bfloat16), "dy": (loud * dy * (SEQUENCES * TOKENS) ** -0.5).astype(jnp.bfloat16)}
    for key, name in zip(kw, NAMES, strict=True):
        w = jax.random.normal(key, SHAPES[name], jnp.float32) * SHAPES[name][1] ** -0.5
        drawn[name] = (w * {"w_gate": 1.0, "w_up": bump(kh, FF, 4.0), "w_down": layers}[name]).astype(jnp.bfloat16)
    for key, name in zip(km, NAMES, strict=True):
        drawn[f"m_{name}"] = 0.1 * jax.random.normal(key, SHAPES[name], jnp.float32)
    for key, name in zip(kv, NAMES, strict=True):
        drawn[f"v_{name}"] = jax.random.uniform(key, SHAPES[name], jnp.float32, 0.005, 0.015)
    return drawn


def matmul(a, w):
    return jnp.dot(a, w, preferred_element_type=jnp.float32).astype(jnp.bfloat16)


def normed(h):
    wide = h.astype(jnp.float32)
    scale = lax.rsqrt(jnp.mean(wide**2, -1, keepdims=True) + 1e-6)
    return (wide * scale).astype(jnp.bfloat16)


def layer(h, w):
    a = normed(h)
    gate = jnp.dot(a, w["w_gate"], preferred_element_type=jnp.float32)
    up = jnp.dot(a, w["w_up"], preferred_element_type=jnp.float32)
    return h + matmul((jax.nn.silu(gate) * up).astype(jnp.bfloat16), w["w_down"])


def adamw(w, m, v, g):
    m = 0.9 * m + 0.1 * g
    v = 0.95 * v + 0.05 * g * g
    step = m * lax.rsqrt(v + 1e-8) + 0.1 * w
    return (w - 0.02 * step).astype(jnp.bfloat16), m, v


def clipped(gradients, sum_of_squares, count):
    factor = jnp.minimum(1.0, 0.5 * lax.rsqrt(sum_of_squares / count + 1e-30))
    return [g * factor for g in gradients]


def stack(weights, h):
    return lax.scan(lambda h, w: (layer(h, w), None), h, weights)[0]


def reference(x, dy, w_gate, w_up, w_down, m_w_gate, m_w_up, m_w_down, v_w_gate, v_w_up, v_w_down):
    weights = dict(zip(NAMES, (w_gate, w_up, w_down), strict=True))

    def take(so_far, sequence):
        h, by_y = sequence
        _, back = jax.vjp(lambda w: stack(w, h), weights)
        return jax.tree.map(lambda total, term: total + term.astype(jnp.float32), so_far, back(by_y)[0]), None

    none_yet = {name: jnp.zeros(w.shape, jnp.float32) for name, w in weights.items()}
    by_weights, _ = lax.scan(take, none_yet, (x, dy))
    gradients = [by_weights[name].astype(jnp.bfloat16).astype(jnp.float32) for name in NAMES]
    gradients = clipped(gradients, sum(jnp.sum(g * g) for g in gradients), sum(g.size for g in gradients))
    new = [
        adamw(w.astype(jnp.float32), m, v, g)
        for w, m, v, g in zip((w_gate, w_up, w_down), (m_w_gate, m_w_up, m_w_down), (v_w_gate, v_w_up, v_w_down), gradients, strict=True)
    ]
    return tuple(one[which] for which in range(3) for one in new)
```

```python
import functools

import jax
import jax.numpy as jnp
from jax import lax
from jax.experimental import pallas as pl
from jax.experimental.pallas import tpu as pltpu
from jax.sharding import PartitionSpec as P

MESH = pl.DeviceIdType.MESH
BF, F32 = jnp.bfloat16, jnp.float32
ANY = pl.BlockSpec(memory_space=pl.ANY)
NN = (((1,), (0,)), ((), ()))
NT = (((1,), (1,)), ((), ()))
TN = (((0,), (0,)), ((), ()))
N, D, FF = 4096, 1024, 2816
C = 256
NC = FF // C
T, S = 1024, 2
R = T // S
TRIPS = N // T


def dot(a, b, how):
    return lax.dot_general(a, b, how, preferred_element_type=F32)


def ds(start, size):
    return pl.ds(pl.multiple_of(start, size), size)


def up(v):
    return v.astype(F32)


def normed_rows(ref, row, size=64):
    def block(i, _):
        rows = ds(row + i * size, size)
        wide = up(ref[rows, :])
        scale = lax.rsqrt(jnp.mean(wide * wide, -1, keepdims=True) + 1e-6)
        ref[rows, :] = (wide * scale).astype(BF)
        return 0

    lax.fori_loop(0, T // size, block, 0)


def forward_kernel(x_hbm, wg_hbm, wu_hbm, wd_hbm, h_hbm, a_hbm, gate_hbm, up_hbm,
                   a, acc, wg, wu, wd, gt, ut, act, xt, isem, wsem, osem, hsem):
    def loads(p, slot):
        return [pltpu.make_async_copy(src.at[p], dst.at[slot], wsem.at[slot, i])
                for i, (src, dst) in enumerate(((wg_hbm, wg), (wu_hbm, wu), (wd_hbm, wd)))]

    def saves(p, t, slot):
        rows = ds(t * T, T)
        return [pltpu.make_async_copy(src.at[slot], dst.at[p, rows], osem.at[slot, i])
                for i, (src, dst) in enumerate(((gt, gate_hbm), (ut, up_hbm)))]

    xin = [pltpu.make_async_copy(x_hbm.at[pl.ds(t * T, T)], a.at[pl.ds(t * T, T)], isem.at[t]) for t in range(TRIPS)]
    for copy in xin:
        copy.start()
    for copy in loads(0, 0):
        copy.start()
    for t in range(TRIPS):
        xin[t].wait()
        normed_rows(a, t * T)
    aout = pltpu.make_async_copy(a, a_hbm, isem.at[TRIPS])
    aout.start()

    def chunk(p, _):
        w = lax.rem(p, 2)
        for copy in loads(p, w):
            copy.wait()

        @pl.when(p + 1 < NC)
        def _():
            for copy in loads(p + 1, 1 - w):
                copy.start()

        def trip(t, _):
            o = lax.rem(t, 2)

            @pl.when(p * TRIPS + t >= 2)
            def _():
                for copy in saves(0, 0, o):
                    copy.wait()

            def rows(i):
                return ds(t * T + i * R, R)

            def first(i):
                at = a[rows(i), :]
                gt[o, i * R : (i + 1) * R] = dot(at, wg[w], NN)
                ut[o, i * R : (i + 1) * R] = dot(at, wu[w], NN)

            def middle(i):
                g, u = gt[o, i * R : (i + 1) * R], ut[o, i * R : (i + 1) * R]
                act[i] = (g / (1.0 + jnp.exp(-g)) * u).astype(BF)

            def last(i):
                acc[rows(i), :] = jnp.where(p == 0, 0.0, acc[rows(i), :]) + dot(act[i], wd[w], NN)

            first(0)
            for i in range(S):
                if i + 1 < S:
                    first(i + 1)
                middle(i)
                last(i)
            for copy in saves(p, t, o):
                copy.start()

            @pl.when(p == NC - 1)
            def _():
                copy = pltpu.make_async_copy(x_hbm.at[ds(t * T, T)], xt, hsem.at[0])

                @pl.when(t > 0)
                def _():
                    pltpu.make_async_copy(a.at[ds(t * T, T)], h_hbm.at[ds(t * T, T)], hsem.at[1]).wait()

                @pl.when(t == 0)
                def _():
                    pltpu.make_async_copy(a, a_hbm, isem.at[TRIPS]).wait()

                copy.start()
                copy.wait()

                def block(i, _):
                    r = ds(i * 64, 64)
                    q = ds(t * T + i * 64, 64)
                    a[q, :] = (up(xt[r, :]) + up(acc[q, :].astype(BF))).astype(BF)
                    return 0

                lax.fori_loop(0, T // 64, block, 0)
                pltpu.make_async_copy(a.at[ds(t * T, T)], h_hbm.at[ds(t * T, T)], hsem.at[1]).start()

            return 0

        lax.fori_loop(0, TRIPS, trip, 0)
        return 0

    lax.fori_loop(0, NC, chunk, 0)
    for o in range(2):
        for copy in saves(0, 0, o):
            copy.wait()
    pltpu.make_async_copy(a.at[pl.ds(0, T)], h_hbm.at[pl.ds(0, T)], hsem.at[1]).wait()


def forward(x, wg, wu, wd):
    return pl.pallas_call(
        forward_kernel,
        name="forward0",
        in_specs=[ANY] * 4,
        out_specs=[ANY] * 4,
        out_shape=[jax.ShapeDtypeStruct((N, D), BF)] * 2 + [jax.ShapeDtypeStruct((NC, N, C), F32)] * 2,
        scratch_shapes=[
            pltpu.VMEM((N, D), BF), pltpu.VMEM((N, D), F32),
            pltpu.VMEM((2, D, C), BF), pltpu.VMEM((2, D, C), BF), pltpu.VMEM((2, C, D), BF),
            pltpu.VMEM((2, T, C), F32), pltpu.VMEM((2, T, C), F32), pltpu.VMEM((S, R, C), BF), pltpu.VMEM((T, D), BF),
            pltpu.SemaphoreType.DMA((TRIPS + 1,)), pltpu.SemaphoreType.DMA((2, 3)), pltpu.SemaphoreType.DMA((2, 2)), pltpu.SemaphoreType.DMA((2,)),
        ],
        compiler_params=pltpu.CompilerParams(vmem_limit_bytes=62 * 2**20),
    )(x, wg, wu, wd)


def backward_kernel(h_hbm, dy_hbm, wg_hbm, wu_hbm, wd_hbm, wd0_hbm, a0_hbm, gate_hbm, up_hbm,
                    gg_hbm, gu_hbm, gd_hbm, sq_ref,
                    a, dy, da, wg, wu, wd, acc_g, acc_u, acc_d, gt, ut, dt, act, dg, du,
                    send_a, recv_a, own_b, send_b, recv_b, send_c, recv_c, out,
                    isem, wsem, tsem, sa, ra, sb, rb, sc, rc, osem, dsem):
    me, mr = lax.axis_index("s"), lax.axis_index("r")
    x, c = me // 2, lax.rem(me, 2)
    sib, xn, yn = {"s": me + 1 - 2 * c}, {"s": lax.rem(me + 2, 4)}, {"r": 1 - mr}
    barrier = pltpu.get_barrier_semaphore()
    for peer in (sib, xn, yn):
        pl.semaphore_signal(barrier, inc=1, device_id=peer, device_id_type=MESH)
    pl.semaphore_wait(barrier, 3)

    def copy_a(u):
        s = lax.rem(u, 2)
        return pltpu.make_async_remote_copy(send_a, recv_a.at[s], sa, ra.at[s], device_id=sib, device_id_type=MESH)

    def copy_b(u):
        s, q = lax.rem(u, 2), lax.rem(u, 4)
        return pltpu.make_async_remote_copy(send_b.at[s], recv_b.at[q], sb.at[s], rb.at[q], device_id=xn, device_id_type=MESH)

    def copy_c(u):
        s, q = lax.rem(u, 2), lax.rem(u, 4)
        return pltpu.make_async_remote_copy(send_c.at[s], recv_c.at[q], sc.at[s], rc.at[q], device_id=yn, device_id_type=MESH)

    def part(s, m, xd, cc):
        if m < 2:
            return [(slice(0, 256), (acc_g, acc_u)[m][s, ds(512 * xd + 256 * cc, 256), :])]
        return [(slice(128 * k, 128 * k + 128), acc_d[s, ds(128 * xd, 128), ds(512 * cc + 256 * k, 256)]) for k in range(2)]

    def stage_a(u):
        s = lax.rem(u, 2)

        @pl.when(u >= 1)
        def _():
            copy_a(u - 1).wait_send()

        for xd in range(2):
            for m in range(3):
                for rows, term in part(s, m, xd, 1 - c):
                    send_a[xd, m, rows, :] = term.astype(BF)
        copy_a(u).start()

    def stage_b(u):
        s = lax.rem(u, 2)
        copy_a(u).wait_recv()

        @pl.when(u >= 2)
        def _():
            copy_b(u - 2).wait_send()

        for m in range(3):
            for rows, term in part(s, m, 1 - x, c):
                send_b[s, m, rows, :] = (term + up(recv_a[s, 1 - x, m, rows, :])).astype(BF)
        copy_b(u).start()
        for m in range(3):
            for rows, term in part(s, m, x, c):
                own_b[s, m, rows, :] = term + up(recv_a[s, x, m, rows, :])

    def stage_c(u):
        s, q = lax.rem(u, 2), lax.rem(u, 4)
        copy_b(u).wait_recv()

        @pl.when(u >= 2)
        def _():
            copy_c(u - 2).wait_send()

        send_c[s] = (own_b[s] + up(recv_b[q])).astype(BF)
        copy_c(u).start()

    def outs(u, wait):
        s, layer, p = lax.rem(u, 2), 1 - u // NC, lax.rem(u, NC)
        for m, dst in ((0, gg_hbm), (1, gu_hbm)):
            for k in range(2):
                copy = pltpu.make_async_copy(out.at[s, m, :, pl.ds(128 * k, 128)], dst.at[layer, :, ds((p + NC * k) * 128, 128)], osem.at[s, 2 * m + k])
                copy.wait() if wait else copy.start()
        for i in range(2):
            q = 2 * p + i
            owner = q // NC
            for k in range(2):
                src = out.at[s, 2, pl.ds(128 * k + 64 * i, 64), :]
                dst = gd_hbm.at[layer, ds((q - NC * owner) * 64, 64), ds(512 * c + 256 * k, 256)]
                local = pltpu.make_async_copy(src, dst, osem.at[s, 4 + 2 * i + k])
                far = pltpu.make_async_remote_copy(src, dst, osem.at[s, 4 + 2 * i + k], dsem.at[layer], device_id=sib, device_id_type=MESH)

                @pl.when(owner == c)
                def _():
                    local.wait() if wait else local.start()

                @pl.when(owner != c)
                def _():
                    far.wait_send() if wait else far.start()

    def stage_d(u):
        s, q = lax.rem(u, 2), lax.rem(u, 4)
        copy_c(u).wait_recv()

        @pl.when(u >= 2)
        def _():
            outs(u - 2, True)

        total = (up(send_c[s]) + up(recv_c[q])).astype(BF)
        out[s] = total
        wide = up(total)
        sq_ref[...] += jnp.sum((wide * wide).reshape(96, 8, 256), axis=0)
        outs(u, False)

    def comm(u, t):
        @pl.when((t == 0) & (u >= 1))
        def _():
            stage_a(u - 1)

        @pl.when((t == 0) & (u >= 4))
        def _():
            stage_d(u - 4)

        @pl.when((t == 2) & (u >= 1))
        def _():
            stage_b(u - 1)

        @pl.when((t == 3) & (u >= 2))
        def _():
            stage_c(u - 2)

    def loads(p, slot):
        return [pltpu.make_async_copy(src.at[p], dst.at[slot], wsem.at[slot, i])
                for i, (src, dst) in enumerate(((wg_hbm, wg), (wu_hbm, wu), (wd_hbm, wd)))]

    def load0(p, slot):
        return pltpu.make_async_copy(wd0_hbm.at[p], wd.at[slot], wsem.at[slot, 2])

    def saved(p, t):
        s, rows = lax.rem(t, 2), ds(t * T, T)
        return [pltpu.make_async_copy(src.at[p, rows], dst.at[s], tsem.at[s, i]) for i, (src, dst) in enumerate(((gate_hbm, gt), (up_hbm, ut)))]

    def tile(src, dst, t, k):
        return pltpu.make_async_copy(src.at[ds(t * T, T)], dst.at[ds(t * T, T)], isem.at[k, t])

    for t in range(TRIPS):
        tile(h_hbm, a, t, 0).start()
        tile(dy_hbm, dy, t, 1).start()
    for copy in loads(0, 0):
        copy.start()
    sq_ref[...] = jnp.zeros_like(sq_ref)
    for t in range(TRIPS):
        tile(h_hbm, a, t, 0).wait()
        normed_rows(a, t * T)
        tile(dy_hbm, dy, t, 1).wait()

    def pointwise(i, g, u):
        d = up(dt[i].astype(BF))
        sig = 1.0 / (1.0 + jnp.exp(-g))
        silu = g * sig
        act[i] = (silu * u).astype(BF)
        du[i] = (d * silu).astype(BF)
        dg[i] = (d * u * (sig * (1.0 + g * (1.0 - sig)))).astype(BF)

    def weight_grads(u, t):
        s, rows = lax.rem(u, 2), ds(t * T, T)
        at, dyt = a[rows, :], dy[rows, :]
        acc_g[s] = jnp.where(t == 0, 0.0, acc_g[s]) + dot(at, dg[...].reshape(T, C), TN)
        acc_u[s] = jnp.where(t == 0, 0.0, acc_u[s]) + dot(at, du[...].reshape(T, C), TN)
        acc_d[s] = jnp.where(t == 0, 0.0, acc_d[s]) + dot(act[...].reshape(T, C), dyt, TN)

    def norm_back(t):
        def block(i, _):
            rows = ds(t * T + i * 64, 64)
            wide, g = up(a[rows, :]), up(da[rows, :].astype(BF))
            scale = lax.rsqrt(jnp.mean(wide * wide, -1, keepdims=True) + 1e-6)
            inner = jnp.sum(g * wide, -1, keepdims=True) * (scale * scale * scale * (1.0 / D))
            dy[rows, :] = (up(dy[rows, :]) + up((g * scale - wide * inner).astype(BF))).astype(BF)
            return 0

        lax.fori_loop(0, T // 64, block, 0)

    def chunk1(u, _):
        w = lax.rem(u, 2)
        for copy in loads(u, w):
            copy.wait()

        @pl.when(u + 1 < NC)
        def _():
            for copy in loads(u + 1, 1 - w):
                copy.start()

        @pl.when(u + 1 == NC)
        def _():
            load0(0, 1 - w).start()

        def trip(t, _):
            comm(u, t)

            @pl.when((u == NC - 1) & (t > 0))
            def _():
                tile(h_hbm, a, t - 1, 0).wait()
                norm_back(t - 1)
                tile(a0_hbm, a, t - 1, 0).start()

            def rows(i):
                return ds(t * T + i * R, R)

            def first(i):
                at, dyt = a[rows(i), :], dy[rows(i), :]
                gt[i, :R] = dot(at, wg[w], NN)
                ut[i, :R] = dot(at, wu[w], NN)
                dt[i] = dot(dyt, wd[w], NT)

            def last(i):
                da[rows(i), :] = jnp.where(u == 0, 0.0, da[rows(i), :]) + dot(dg[i], wg[w], NT) + dot(du[i], wu[w], NT)

            first(0)
            for i in range(S):
                if i + 1 < S:
                    first(i + 1)
                pointwise(i, gt[i, :R], ut[i, :R])
                last(i)
            weight_grads(u, t)

            @pl.when(u == NC - 1)
            def _():
                tile(h_hbm, a, t, 0).start()

            return 0

        lax.fori_loop(0, TRIPS, trip, 0)
        return 0

    lax.fori_loop(0, NC, chunk1, 0)
    for copy in saved(0, 0):
        copy.start()
    tile(h_hbm, a, TRIPS - 1, 0).wait()
    norm_back(TRIPS - 1)
    tile(a0_hbm, a, TRIPS - 1, 0).start()

    def chunk0(u, _):
        w, p = lax.rem(u, 2), u - NC
        load0(p, w).wait()

        @pl.when(p + 1 < NC)
        def _():
            load0(p + 1, 1 - w).start()

        def trip(t, _):
            comm(u, t)
            o = lax.rem(t, 2)

            @pl.when(p == 0)
            def _():
                tile(a0_hbm, a, t, 0).wait()

            for copy in saved(p, t):
                copy.wait()

            @pl.when((t + 1 < TRIPS) | (p + 1 < NC))
            def _():
                more = (t + 1) // TRIPS
                for copy in saved(p + more, t + 1 - TRIPS * more):
                    copy.start()

            def rows(i):
                return ds(t * T + i * R, R)

            def first(i):
                dt[i] = dot(dy[rows(i), :], wd[w], NT)

            first(0)
            for i in range(S):
                if i + 1 < S:
                    first(i + 1)
                pointwise(i, gt[o, i * R : (i + 1) * R], ut[o, i * R : (i + 1) * R])
            weight_grads(u, t)
            return 0

        lax.fori_loop(0, TRIPS, trip, 0)
        return 0

    lax.fori_loop(NC, 2 * NC, chunk0, 0)

    L = 2 * NC - 1
    stage_a(L)
    stage_d(L - 3)
    stage_b(L)
    stage_c(L - 1)
    stage_d(L - 2)
    stage_c(L)
    stage_d(L - 1)
    stage_d(L)
    copy_a(L).wait_send()
    for u in (L - 1, L):
        copy_b(u).wait_send()
        copy_c(u).wait_send()
        outs(u, True)
    for layer in range(2):
        got = gd_hbm.at[layer, :, ds(512 * (1 - c), 512)]
        pltpu.make_async_copy(got, got, dsem.at[layer]).wait()


def backward(h, dy, wg, wu, wd, wd0, a0, gate, upw):
    dma = pltpu.SemaphoreType.DMA
    return pl.pallas_call(
        backward_kernel,
        name="backward",
        in_specs=[ANY] * 9,
        out_specs=[ANY] * 3 + [pl.BlockSpec(memory_space=pltpu.VMEM)],
        out_shape=[jax.ShapeDtypeStruct((2, 256, FF), BF)] * 2 + [jax.ShapeDtypeStruct((2, FF // 4, D), BF), jax.ShapeDtypeStruct((8, 256), F32)],
        scratch_shapes=[
            pltpu.VMEM((N, D), BF), pltpu.VMEM((N, D), BF), pltpu.VMEM((N, D), F32),
            pltpu.VMEM((2, D, C), BF), pltpu.VMEM((2, D, C), BF), pltpu.VMEM((2, C, D), BF),
            pltpu.VMEM((2, D, C), F32), pltpu.VMEM((2, D, C), F32), pltpu.VMEM((2, C, D), F32),
            pltpu.VMEM((2, T, C), F32), pltpu.VMEM((2, T, C), F32), pltpu.VMEM((S, R, C), F32),
            pltpu.VMEM((S, R, C), BF), pltpu.VMEM((S, R, C), BF), pltpu.VMEM((S, R, C), BF),
            pltpu.VMEM((2, 3, 256, 256), BF), pltpu.VMEM((2, 2, 3, 256, 256), BF), pltpu.VMEM((2, 3, 256, 256), F32),
            pltpu.VMEM((2, 3, 256, 256), BF), pltpu.VMEM((4, 3, 256, 256), BF),
            pltpu.VMEM((2, 3, 256, 256), BF), pltpu.VMEM((4, 3, 256, 256), BF), pltpu.VMEM((2, 3, 256, 256), BF),
            dma((2, TRIPS)), dma((2, 3)), dma((2, 2)),
            dma(()), dma((2,)), dma((2,)), dma((4,)), dma((2,)), dma((4,)), dma((2, 8)), dma((2,)),
        ],
        compiler_params=pltpu.CompilerParams(vmem_limit_bytes=63 * 2**20, collective_id=0, has_side_effects=True),
    )(h, dy, wg, wu, wd, wd0, a0, gate, upw)


def adamw(w, m, v, g):
    m = 0.9 * m + 0.1 * g
    v = 0.95 * v + 0.05 * g * g
    step = m * lax.rsqrt(v + 1e-8) + 0.1 * w
    return (w - 0.02 * step).astype(BF), m, v


def solution(mesh):
    def columns(w):
        whole = lax.all_gather(w, "s", axis=0, tiled=True)
        return whole.reshape(D, 2, NC, 128).transpose(2, 0, 1, 3).reshape(NC, D, C)

    def rows(w):
        whole = lax.all_gather(w, "s", axis=0, tiled=True)
        return whole.reshape(2, NC, 128, D).transpose(1, 0, 2, 3).reshape(NC, C, D)

    def step(x, dy, *arrays):
        weights, m, v = (arrays[i : i + 3] for i in (0, 3, 6))
        wg, wu, wd = ([how(w[number]) for number in range(2)] for how, w in zip((columns, columns, rows), weights))
        h, a0, gate, upw = forward(x[0], wg[0], wu[0], wd[0])
        *gradients, sq = backward(h, dy[0], wg[1], wu[1], wd[1], wd[0], a0, gate, upw)
        squares = lax.psum(jnp.sum(sq), "s")
        count = 6.0 * D * FF
        factor = jnp.minimum(1.0, 0.5 * lax.rsqrt(squares / count + 1e-30))
        new = [adamw(up(w), m, v, up(g) * factor) for w, m, v, g in zip(weights, m, v, gradients, strict=True)]
        return tuple(one[which] for which in range(3) for one in new)

    states, cut = P(("rep", "r", "s"), None, None), P(None, "s", None)
    return jax.shard_map(
        step,
        mesh=mesh,
        in_specs=(states, states) + (cut,) * 9,
        out_specs=(P("rep", "s", None),) * 9,
        check_vma=False,
    )
```

```python
import functools

import jax
import jax.numpy as jnp
from jax import lax
from jax.experimental import pallas as pl
from jax.experimental.pallas import tpu as pltpu
from jax.sharding import PartitionSpec as P

MESH = pl.DeviceIdType.MESH
BF, F32 = jnp.bfloat16, jnp.float32
ANY = pl.BlockSpec(memory_space=pl.ANY)
NN = (((1,), (0,)), ((), ()))
NT = (((1,), (1,)), ((), ()))
TN = (((0,), (0,)), ((), ()))
PAIR, THREE = range(2), range(3)
N, D, FF = 4096, 1024, 2816
STRIP, PART = 128, 64
C = 2 * STRIP
NC = FF // C
R = 512
T = 2 * R
TRIPS, TILES = N // T, N // R
WIDE = 4
LONG = WIDE * R
HALF = D // 2
ROWS, PB = 16, 32
EPS = 1e-6
EARLY, AT = 4, 13


def dot(a, b, how):
    return lax.dot_general(a, b, how, preferred_element_type=F32)


def ds(start, size):
    return pl.ds(pl.multiple_of(start, size), size)


def up(v):
    return v.astype(F32)


def odd(v):
    return lax.rem(v, 2)


def loop(first, last, body):
    def step(i, nothing):
        body(i)
        return nothing

    lax.fori_loop(first, last, step, 0)


def passes(count, prepare, finish, unroll):
    def step(i):
        parts = [ds((i * unroll + k) * ROWS, ROWS) for k in range(unroll)]
        ready = [prepare(rows) for rows in parts]
        for rows, value in zip(parts, ready):
            finish(rows, value)

    loop(0, count // (ROWS * unroll), step)


def before(j, u):
    return jnp.where(j == 0, TILES - 1, j - 1), jnp.where(j == 0, u - 1, u)


def scale_of(wide):
    return lax.rsqrt(jnp.mean(wide * wide, -1, keepdims=True) + EPS)


class Gather:
    def __init__(self, layer, shards, gu, wd, sems, sends, halves):
        self.layer, self.shards, self.gu, self.wd, self.halves = layer, shards, gu, wd, halves
        self.sems, self.sends = sems, sends
        self.me, self.y = lax.axis_index("s"), lax.axis_index("r")
        self.x, self.c = self.me // 2, odd(self.me)
        self.sib, self.xn = self.me + 1 - 2 * self.c, lax.rem(self.me + 2, 4)
        self.diagonal = self.xn + 1 - 2 * self.c
        self.peers = {"sib": {"s": self.sib}, "xn": {"s": self.xn}, "yn": {"r": 1 - self.y}, "diagonal": {"s": self.diagonal}}
        self.whole = (0, C)

    def far(self, src, dst, kind, where, which):
        row = kind % 5
        sem = self.sems[kind // 5].at[row if self.halves else (row + 1) // 2, where]
        return pltpu.make_async_remote_copy(src, dst, self.sends.at[kind], sem, device_id=self.peers[which], device_id_type=MESH)

    def strips(self, p, part):
        start, size = part
        for m in PAIR:
            for k in PAIR:
                yield (self.shards[m].at[self.layer, ds(start, size), ds((p + NC * k) * STRIP, STRIP)],
                       self.gu.at[p, m, ds(C * self.me + start, size), pl.ds(STRIP * k, STRIP)])

    def block(self, p, owner, part):
        start, size = part
        return self.gu.at[p, :, ds(C * owner + start, size), :]

    def owner(self, p, i):
        return (2 * p + i) // NC

    def shard_rows(self, p, i):
        return self.shards[2].at[self.layer, ds((2 * p + i - NC * self.c) * PART, PART), :]

    def rows(self, p, i, x, half=None):
        rows = ds(STRIP * x + PART * i, PART)
        return self.wd.at[p, rows, :] if half is None else self.wd.at[p, rows, ds(HALF * half, HALF)]

    def mine(self, p, i, yes, no=None):
        pl.when(self.owner(p, i) == self.c)(yes)
        if no is not None:
            pl.when(self.owner(p, i) != self.c)(no)

    def part(self, h):
        return (STRIP * h, STRIP) if self.halves else self.whole

    def half(self, h):
        return h if self.halves else None

    def issue(self, p):
        for src, dst in self.strips(p, self.part(self.y)):
            self.far(src, dst, 1, p, "xn").start()
        for src, dst in self.strips(p, self.whole):
            self.far(src, dst, 0, p, "sib").start()
        for i in PAIR:
            def send(i=i):
                src = self.shard_rows(p, i)
                self.far(src, self.rows(p, i, self.x), 5, 2 * p + i, "sib").start()
                if self.halves:
                    src = src.at[:, ds(HALF * self.y, HALF)]
                self.far(src, self.rows(p, i, self.x, self.half(self.y)), 6, 2 * p + i, "xn").start()
            self.mine(p, i, send)

    def pass_on(self, p):
        block = self.block(p, self.xn, self.part(self.y))
        self.far(block, block, 1, p, "xn").wait_recv()
        if self.halves:
            self.far(block, block, 2, p, "yn").start()
        self.far(block, block, 3, p, "sib").start()
        for i in PAIR:
            def send(i=i):
                rows = self.rows(p, i, 1 - self.x, self.half(self.y))
                self.far(rows, rows, 6, 2 * p + i, "xn").wait_recv()
                if self.halves:
                    self.far(rows, rows, 7, 2 * p + i, "yn").start()
                self.far(rows, rows, 8, 2 * p + i, "sib").start()
            self.mine(p, i, send)

    def pass_on_y(self, p):
        block = self.block(p, self.xn, self.part(1 - self.y))
        self.far(block, block, 2, p, "yn").wait_recv()
        self.far(block, block, 4, p, "sib").start()
        for i in PAIR:
            def send(i=i):
                rows = self.rows(p, i, 1 - self.x, 1 - self.y)
                self.far(rows, rows, 7, 2 * p + i, "yn").wait_recv()
                self.far(rows, rows, 9, 2 * p + i, "sib").start()
            self.mine(p, i, send)

    def arrived(self, p):
        block = self.block(p, self.sib, self.whole)
        self.far(block, block, 0, p, "sib").wait_recv()
        ways = ((3, 8, self.y), (4, 9, 1 - self.y)) if self.halves else ((3, 8, self.y),)
        for kind, _, h in ways:
            block = self.block(p, self.diagonal, self.part(h))
            self.far(block, block, kind, p, "sib").wait_recv()
        for i in PAIR:
            def wait(i=i):
                rows = self.rows(p, i, self.x)
                self.far(rows, rows, 5, 2 * p + i, "sib").wait_recv()
                for _, kind, h in ways:
                    rows = self.rows(p, i, 1 - self.x, self.half(h))
                    self.far(rows, rows, kind, 2 * p + i, "sib").wait_recv()
            pl.when(self.owner(p, i) != self.c)(wait)

    def finish(self):
        for kind in (range(10) if self.halves else (0, 1, 3, 5, 6, 8)):
            all_rows = kind in (0, 5) or not self.halves
            if kind < 5:
                block = self.gu.at[:, :, pl.ds(0, C if all_rows else STRIP), :]
            else:
                block = self.wd.at[:, pl.ds(0, PART), :] if all_rows else self.wd.at[:, pl.ds(0, PART), pl.ds(0, HALF)]
            self.far(block, block, kind, 0, "sib").wait_send()


def kernel(x_hbm, dy_hbm, w_gate, w_up, w_down,
           h_hbm, a0_hbm, gate_hbm, up_hbm, wd0_hbm, gu1_hbm, wd1_hbm, gg_hbm, gu_hbm, gd_hbm, factor_ref,
           a, da, act0, act1, sq, sqs,
           isem, osem, tsem, wsem, xsem, own, gsem0, dsem0, sends0, gsem1, dsem1, sends1, outs_sem, dsem, ra, rb, rc, sa, sb, sc, fsem, inside):
    shards = (w_gate, w_up, w_down)
    act = (act0, act1)
    g1 = Gather(1, shards, gu1_hbm, wd1_hbm, (gsem1, dsem1), sends1, False)
    me, x, c, peers = g1.me, g1.x, g1.c, g1.peers

    def move(src, dst, sem):
        return pltpu.make_async_copy(src, dst, sem)

    def first_layer(gu, wd, xt, gt, ut):
        g0 = Gather(0, shards, gu, wd, (gsem0, dsem0), sends0, True)

        def saves(p, t, slot):
            return [move(src.at[slot], dst.at[p, ds(t * LONG, LONG)], osem.at[slot, i]) for i, (src, dst) in enumerate(((gt, gate_hbm), (ut, up_hbm)))]

        def local(p, wait):
            if wait:
                block = g0.block(p, me, g0.whole)
                move(block, block, own.at[p, 2]).wait()
            else:
                for src, dst in g0.strips(p, g0.whole):
                    move(src, dst, own.at[p, 2]).start()
            for i in PAIR:
                def go(i=i):
                    copy = move(g0.shard_rows(p, i), g0.rows(p, i, x), own.at[p, i])
                    copy.wait() if wait else copy.start()
                g0.mine(p, i, go)

        def keep(p):
            return move(wd.at[p], wd0_hbm.at[p], fsem.at[3])

        xin = [move(x_hbm.at[pl.ds(t * T, T)], a.at[t], isem.at[0, t]) for t in range(TRIPS)]
        turned = [move(xt.at[odd_], a0_hbm.at[t, :, pl.ds(R * odd_, R)], isem.at[1, 2 * t + odd_]) for t in range(TRIPS) for odd_ in PAIR]
        for copy in xin:
            copy.start()
        barrier = pltpu.get_barrier_semaphore()
        for peer in peers.values():
            pl.semaphore_signal(barrier, inc=1, device_id=peer, device_id_type=MESH)
        pl.semaphore_wait(barrier, len(peers))

        def issue0(p):
            g0.issue(p)
            local(p, False)

        def issue1(p):
            g1.issue(p)

        loop(0, 2, issue0)
        for t in range(TRIPS):
            xin[t].wait()

            def put(rows, scale):
                a[t, rows, :] = (up(a[t, rows, :]) * scale).astype(BF)

            passes(T, lambda rows: scale_of(up(a[t, rows, :])), put, 8)
            for h in PAIR:
                if t >= 1:
                    turned[2 * t + h - 2].wait()
                for k in PAIR:
                    xt[h, :, C * k : C * (k + 1)] = a[t, R * h + C * k : R * h + C * (k + 1), :].T
                turned[2 * t + h].start()
            if t == 0:
                loop(2, NC, issue0)
            if t == 1:
                g0.pass_on(0)
            if t == 2:
                g0.pass_on(1)
                loop(0, NC, issue1)
        g0.pass_on_y(0)

        def down(i, j, p):
            rows = ds(j * R, R)
            da[rows, :] = jnp.where(p == 0, 0.0, da[rows, :]) + dot(act[i][...], wd[jnp.maximum(p, 0)], NN)

        def chunk(p):
            def trip(t):
                now = 2 * p + t

                @pl.when((now >= 1) & (now + 1 < NC))
                def _():
                    g0.pass_on(now + 1)

                @pl.when((now == 1) | (now >= 3) & (now <= NC))
                def _():
                    g0.pass_on_y(jnp.maximum(now - 1, 1))

                early = (2 * (now - AT) + 4) // 5

                @pl.when((now >= AT) & ((5 * early) // 2 == now - AT) & (early < EARLY))
                def _():
                    g1.pass_on(early)

                @pl.when(t == 0)
                def _():
                    local(p, True)
                    g0.arrived(p)
                    keep(p).start()

                @pl.when(now >= 2)
                def _():
                    for copy in saves(0, 0, t):
                        copy.wait()

                for i in range(WIDE):
                    part, j = pl.ds(i * R, R), WIDE * t + i
                    at = a[2 * t + i // 2, i % 2 * R : (i % 2 + 1) * R, :]
                    gt[t, part] = dot(at, gu[p, 0], NN)
                    ut[t, part] = dot(at, gu[p, 1], NN)
                    down(1 - i % 2, *before(j, p))
                    for k in range(0, R, PB):
                        g, u = gt[t, pl.ds(i * R + k, PB)], ut[t, pl.ds(i * R + k, PB)]
                        act[i % 2][k : k + PB] = (g / (1.0 + jnp.exp(-g)) * u).astype(BF)
                for copy in saves(p, t, t):
                    copy.start()

            loop(0, N // LONG, trip)

        loop(0, NC, chunk)
        down(1, TILES - 1, NC - 1)
        for copy in turned[-2:]:
            copy.wait()
        for o in PAIR:
            for copy in saves(0, 0, o):
                copy.wait()
        move(wd, wd0_hbm, fsem.at[3]).wait()
        g0.finish()

    pl.run_scoped(first_layer, pltpu.VMEM((NC, 2, D, C), BF), pltpu.VMEM((NC, C, D), BF), pltpu.VMEM((2, D, R), BF), *[pltpu.VMEM((2, LONG, C), F32)] * 2)

    def rest(dy, wgu, wd, acc_g, acc_u, acc_d, gt, ut, dt, dg0, dg1, du0, du1, ht,
             send_a, recv_a, own_b, send_b, recv_b, send_c, recv_c, out_gu, out_d):
        dg, du = (dg0, dg1), (du0, du1)

        def copy_a(u):
            return pltpu.make_async_remote_copy(send_a, recv_a.at[odd(u)], sa, ra.at[odd(u)], device_id=peers["sib"], device_id_type=MESH)

        def copy_b(u):
            s, q = odd(u), lax.rem(u, 4)
            return pltpu.make_async_remote_copy(send_b.at[s], recv_b.at[q], sb.at[s], rb.at[q], device_id=peers["xn"], device_id_type=MESH)

        def copy_c(u):
            s, q = odd(u), lax.rem(u, 4)
            return pltpu.make_async_remote_copy(send_c.at[s], recv_c.at[q], sc.at[s], rc.at[q], device_id=peers["yn"], device_id_type=MESH)

        def outs(u, wait):
            s, layer, p = odd(u), 1 - u // NC, lax.rem(u, NC)

            def go(copy, far=False):
                (copy.wait_send if far else copy.wait)() if wait else copy.start()

            for m, dst in enumerate((gg_hbm, gu_hbm)):
                for k in PAIR:
                    go(move(out_gu.at[s, m, :, pl.ds(STRIP * k, STRIP)], dst.at[layer, :, ds((p + NC * k) * STRIP, STRIP)], outs_sem.at[s, 2 * m + k]))
            for i in PAIR:
                q, sem = 2 * p + i, outs_sem.at[s, 4 + i]
                owner = g1.owner(p, i)
                src = out_d.at[s, pl.ds(PART * i, PART), :]
                dst = gd_hbm.at[layer, ds((q - NC * owner) * PART, PART), ds(HALF * c, HALF)]
                g1.mine(p, i, lambda: go(move(src, dst, sem)),
                        lambda: go(pltpu.make_async_remote_copy(src, dst, sem, dsem.at[layer], device_id=peers["sib"], device_id_type=MESH), True))

        def part(s, m, xd, cc):
            if m < 2:
                return [(pl.ds(0, C), (acc_g, acc_u)[m][s, ds(2 * C * xd + C * cc, C), :])]
            return [(pl.ds(STRIP * k, STRIP), acc_d[s, ds(STRIP * xd, STRIP), ds(HALF * cc + C * k, C)]) for k in PAIR]

        def stage_a(u):
            @pl.when(u >= 1)
            def _():
                copy_a(u - 1).wait_send()

            for xd in PAIR:
                for m in THREE:
                    for rows, term in part(odd(u), m, xd, 1 - c):
                        send_a[xd, m, rows, :] = term.astype(BF)
            copy_a(u).start()

        def stage_b(u):
            s = odd(u)
            copy_a(u).wait_recv()

            @pl.when(u >= 2)
            def _():
                copy_b(u - 2).wait_send()

            for m in THREE:
                for rows, term in part(s, m, 1 - x, c):
                    send_b[s, m, rows, :] = (term + up(recv_a[s, 1 - x, m, rows, :])).astype(BF)
            copy_b(u).start()
            for m in THREE:
                for rows, term in part(s, m, x, c):
                    own_b[s, m, rows, :] = term + up(recv_a[s, x, m, rows, :])

        def stage_c(u):
            s = odd(u)
            copy_b(u).wait_recv()

            @pl.when(u >= 2)
            def _():
                copy_c(u - 2).wait_send()

            for m in THREE:
                send_c[s, m] = (own_b[s, m] + up(recv_b[lax.rem(u, 4), m])).astype(BF)
            copy_c(u).start()

        def stage_d(u):
            s = odd(u)
            copy_c(u).wait_recv()

            @pl.when(u >= 2)
            def _():
                outs(u - 2, True)

            for m in THREE:
                total = (up(send_c[s, m]) + up(recv_c[lax.rem(u, 4), m])).astype(BF)
                if m < 2:
                    out_gu[s, m] = total
                else:
                    for k in PAIR:
                        out_d[s, :, C * k : C * (k + 1)] = total[STRIP * k : STRIP * (k + 1)]
                sq[...] += jnp.sum((up(total) * up(total)).reshape(C // 8, 8, C), axis=0)
            outs(u, False)

        def travel(u, event, when):
            for stage, lag in (((stage_c, 3),), ((stage_a, 1), (stage_d, 4)), ((stage_b, 1),))[event]:
                @pl.when(when & (u >= lag))
                def _():
                    stage(u - lag)

        def loads(p, slot, wait):
            def go(src, dst, k):
                copy = move(src, dst, wsem.at[slot, k])
                copy.wait() if wait else copy.start()

            for m in PAIR:
                for k in PAIR:
                    go(shards[m].at[1, :, ds((p + NC * k) * STRIP, STRIP)], wgu.at[slot, m, ds(C * me, C), pl.ds(STRIP * k, STRIP)], 2 * m + k)
            for k, owner in enumerate((g1.sib, g1.xn, g1.diagonal)):
                go(g1.block(p, owner, g1.whole), wgu.at[slot, :, ds(C * owner, C), :], 4 + k)
            for i in PAIR:
                there = wd.at[slot, ds(STRIP * x + PART * i, PART), :]
                g1.mine(p, i, lambda: go(g1.shard_rows(p, i), there, 7 + i), lambda: go(g1.rows(p, i, x), there, 7 + i))
            go(wd1_hbm.at[p, ds(STRIP * (1 - x), STRIP), :], wd.at[slot, ds(STRIP * (1 - x), STRIP), :], 9)

        def load0(p, slot):
            return move(wd0_hbm.at[p], wd.at[slot], wsem.at[slot, 10])

        def saved(p, t):
            s = odd(t)
            return [move(src.at[p, ds(t * T, T)], da.at[ds(s * T, T), pl.ds(C * i, C)], tsem.at[s, i]) for i, src in enumerate((gate_hbm, up_hbm))]

        def dyin(t):
            return move(dy_hbm.at[ds(t * T, T)], dy.at[ds(t * T, T)], isem.at[0, t])

        def new(t):
            return move(a0_hbm.at[t], a.at[t], isem.at[1, t])

        def tile(hbm, j, back=False):
            k = lax.rem(j, 4)
            there, here = hbm.at[ds(j * R, R)], ht.at[k]
            return move(here, there, xsem.at[1, k]) if back else move(there, here, xsem.at[0, k])

        neighbours = ("sib", "xn", "yn")
        for which in neighbours:
            pl.semaphore_signal(inside, inc=1, device_id=peers[which], device_id_type=MESH)
        for j in range(4):
            tile(x_hbm, j).start()
        g1.arrived(0)
        loads(0, 0, False)
        for t in range(TRIPS):
            dyin(t).start()
        sq[...] = jnp.zeros_like(sq)

        def output(j):
            tile(x_hbm, j).wait()
            k, t, h = lax.rem(j, 4), j // 2, odd(j)

            def sums(rows):
                value = (up(ht[k, rows, :]) + up(da[ds(j * R + rows.start, ROWS), :].astype(BF))).astype(BF)
                ht[k, rows, :] = value
                return scale_of(up(value))

            def put(rows, scale):
                a[t, ds(h * R + rows.start, ROWS), :] = (up(ht[k, rows, :]) * scale).astype(BF)

            passes(R, sums, put, 8)
            tile(h_hbm, j, True).start()

        def norm_back(j):
            tile(h_hbm, j).wait()
            k = lax.rem(j, 4)

            def parts(part):
                rows = ds(j * R + part.start, ROWS)
                return rows, up(ht[k, part, :]), up(da[rows, :].astype(BF))

            def sums(part):
                _, wide, g = parts(part)
                scale = scale_of(wide)
                return scale, jnp.sum(g * wide, -1, keepdims=True) * (scale * scale * scale * (1.0 / D))

            def put(part, value):
                rows, wide, g = parts(part)
                scale, inner = value
                dy[rows, :] = (up(dy[rows, :]) + up((g * scale - wide * inner).astype(BF))).astype(BF)

            passes(R, sums, put, 4)

            @pl.when(odd(j) == 1)
            def _():
                new(j // 2).start()

            @pl.when(j + 4 < TILES)
            def _():
                tile(h_hbm, j + 4).start()

        def pointwise(i, gate_and_up):
            for k in range(0, R, PB):
                rows = slice(k, k + PB)
                (g, u), d = gate_and_up(k), up(dt[i, rows].astype(BF))
                sig = 1.0 / (1.0 + jnp.exp(-g))
                silu = g * sig
                act[i][rows] = (silu * u).astype(BF)
                du[i][rows] = (d * silu).astype(BF)
                dg[i][rows] = (d * u * (sig + silu * (1.0 - sig))).astype(BF)

        def input_grads(i, j, u, row=None):
            w, rows = odd(u + 2), ds((j if row is None else row) * R, R)
            da[rows, :] = jnp.where(u == 0, 0.0, da[rows, :]) + dot(dg[i][...], wgu[w, 0], NT) + dot(du[i][...], wgu[w, 1], NT)

        def weight_grads(i, j, u, turned=False, block=None):
            s, k, part = odd(u + 2), j // 2 if block is None else block, slice(i * R, (i + 1) * R)
            dyt = dy[ds((2 * k + i) * R, R), :]
            at, how = (a[k, :, part], NN) if turned else (a[k, part, :], TN)
            acc_g[s] = jnp.where(j == 0, 0.0, acc_g[s]) + dot(at, dg[i][...], how)
            acc_u[s] = jnp.where(j == 0, 0.0, acc_u[s]) + dot(at, du[i][...], how)
            acc_d[s] = jnp.where(j == 0, 0.0, acc_d[s]) + dot(act[i][...], dyt, TN)

        def chunk1(u):
            w = odd(u)
            loads(u, w, True)

            @pl.when(u == NC - 1)
            def _():
                for j in range(4):
                    tile(h_hbm, j).start()

            def trip(t):
                now = 2 * u + t
                first, last = u == 0, u == NC - 1
                travel(u, 0, t == 0)
                travel(u, 1, t == 1)

                @pl.when(first)
                def _():
                    for i in range(WIDE):
                        output(WIDE * t + i)
                    for i in PAIR:
                        dyin(2 * t + i).wait()

                @pl.when(now == 2)
                def _():
                    pl.semaphore_wait(inside, len(neighbours))
                    for j in range(TILES - WIDE, TILES):
                        tile(h_hbm, j, True).wait()

                @pl.when(EARLY + now < NC)
                def _():
                    g1.pass_on(EARLY + now)

                @pl.when((t == 1) & (u + 1 < NC))
                def _():
                    g1.arrived(u + 1)
                    loads(u + 1, 1 - w, False)

                @pl.when((t == 1) & last)
                def _():
                    load0(0, 1 - w).start()
                    for j in range(WIDE - 1):
                        norm_back(j)
                    for copy in saved(0, 0):
                        copy.start()

                for i in range(WIDE):
                    j, b, part = WIDE * t + i, i % 2, slice(i % 2 * R, (i % 2 + 1) * R)
                    at, dyt = a[2 * t + i // 2, part, :], dy[ds(j * R, R), :]
                    gt[b] = dot(at, wgu[w, 0], NN)
                    ut[b] = dot(at, wgu[w, 1], NN)
                    dt[b] = dot(dyt, wd[w], NT)
                    pj, pu = before(j, u)
                    nothing = (now == 0) & (i == 0)
                    input_grads(1 - b, pj, pu, jnp.where(nothing, 0, pj))
                    weight_grads(1 - b, pj, pu, False, jnp.where(nothing, 0, pj // 2))
                    pointwise(b, lambda k: (gt[b, k : k + PB], ut[b, k : k + PB]))

                @pl.when(now == 0)
                def _():
                    for j in range(WIDE):
                        tile(h_hbm, j, True).wait()
                        tile(x_hbm, j + WIDE).start()

                travel(u, 2, t == 1)

            loop(0, N // LONG, trip)

        loop(0, NC, chunk1)
        input_grads(1, TILES - 1, NC - 1)
        weight_grads(1, TILES - 1, NC - 1)
        for j in range(WIDE - 1, TILES):
            norm_back(j)
        for ref in (act1, dg1, du1):
            ref[...] = jnp.zeros_like(ref)

        def chunk0(u):
            w, p = odd(u), u - NC
            load0(p, w).wait()

            @pl.when(p + 1 < NC)
            def _():
                load0(p + 1, 1 - w).start()

            def trip(t):
                travel(u, 0, t == 0)
                travel(u, 1, t == 1)
                travel(u, 2, t == TRIPS - 1)

                @pl.when(p == 0)
                def _():
                    new(t).wait()

                for copy in saved(p, t):
                    copy.wait()

                @pl.when((t + 1 < TRIPS) | (p + 1 < NC))
                def _():
                    more = (t + 1) // TRIPS
                    for copy in saved(p + more, t + 1 - TRIPS * more):
                        copy.start()

                for i in PAIR:
                    j = 2 * t + i
                    dt[i] = dot(dy[ds(j * R, R), :], wd[w], NT)
                    pj, pu = before(j, u)
                    weight_grads(1 - i, pj, pu, True, jnp.where((p == 0) & (j == 0), 0, pj // 2))

                    def gate_and_up(k):
                        rows = ds(odd(t) * T + i * R + k, PB)
                        return da[rows, :C], da[rows, C : 2 * C]

                    pointwise(i, gate_and_up)

            loop(0, TRIPS, trip)

        loop(NC, 2 * NC, chunk0)
        weight_grads(1, TILES - 1, 2 * NC - 1, True)

        L = 2 * NC - 1
        for stage, u in ((stage_a, L), (stage_c, L - 2), (stage_d, L - 3), (stage_b, L), (stage_c, L - 1), (stage_d, L - 2), (stage_c, L), (stage_d, L - 1), (stage_d, L)):
            stage(u)
        copy_a(L).wait_send()
        for u in (L - 1, L):
            copy_b(u).wait_send()
            copy_c(u).wait_send()
        sqs[me] = sq[:, :STRIP] + sq[:, STRIP:]
        others = [pltpu.make_async_remote_copy(sqs.at[me], sqs.at[me], fsem.at[k], dsem.at[2 + k], device_id=peers[which], device_id_type=MESH)
                  for k, which in enumerate(("sib", "xn", "diagonal"))]
        for copy in others:
            copy.start()
        g1.finish()
        for copy in others:
            copy.wait()
        mean = jnp.sum(sqs[...]) / (3.0 * 2 * D * FF)
        factor_ref[...] = jnp.full(factor_ref.shape, 1.0) * jnp.minimum(1.0, 0.5 * lax.rsqrt(jnp.full(factor_ref.shape, mean) + 1e-30))
        outs(L - 1, True)
        outs(L, True)
        for layer in PAIR:
            got = gd_hbm.at[layer, :, ds(HALF * (1 - c), HALF)]
            move(got, got, dsem.at[layer]).wait()

    piece, f = (3, C, C), pltpu.VMEM
    pl.run_scoped(
        rest,
        f((N, D), BF), f((2, 2, D, C), BF), f((2, C, D), BF),
        f((2, D, C), F32), f((2, D, C), F32), f((2, C, D), F32),
        *[f((2, R, C), F32)] * 3, *[f((R, C), BF)] * 4, f((4, R, D), BF),
        f((2,) + piece, BF), f((2, 2) + piece, BF), f((2,) + piece, F32),
        f((2,) + piece, BF), f((4,) + piece, BF), f((2,) + piece, BF), f((4,) + piece, BF), f((2, 2, C, C), BF), f((2, STRIP, HALF), BF),
    )


def gradients(x, dy, *shards):
    dma, shape = pltpu.SemaphoreType.DMA, jax.ShapeDtypeStruct
    sides = [[dma((kinds, NC)), dma((kinds, 2 * NC)), dma((10,))] for kinds in (5, 3)]
    return pl.pallas_call(
        kernel,
        name="gradients",
        in_specs=[ANY] * 5,
        out_specs=[ANY] * 10 + [pl.BlockSpec(memory_space=pltpu.VMEM)],
        out_shape=[shape((N, D), BF), shape((TRIPS, D, T), BF), shape((NC, N, C), F32), shape((NC, N, C), F32),
                   shape((NC, C, D), BF), shape((NC, 2, D, C), BF), shape((NC, C, D), BF),
                   shape((2, C, FF), BF), shape((2, C, FF), BF), shape((2, FF // 4, D), BF), shape((8, STRIP), F32)],
        scratch_shapes=[
            pltpu.VMEM((TRIPS, T, D), BF), pltpu.VMEM((N, D), F32),
            pltpu.VMEM((R, C), BF), pltpu.VMEM((R, C), BF), pltpu.VMEM((8, C), F32), pltpu.VMEM((4, 8, STRIP), F32),
            dma((2, TILES)), *[dma((2, 2))] * 2, dma((2, 11)), dma((2, 4)), dma((NC, 3)), *sides[0], *sides[1], dma((2, 6)), dma((5,)),
            dma((2,)), dma((4,)), dma((4,)), dma(()), dma((2,)), dma((2,)), dma((4,)), pltpu.SemaphoreType.REGULAR,
        ],
        compiler_params=pltpu.CompilerParams(vmem_limit_bytes=67_000_000, collective_id=0, has_side_effects=True),
    )(x, dy, *shards)[-4:]


def adamw(w, m, v, g):
    m = 0.9 * m + 0.1 * g
    v = 0.95 * v + 0.05 * g * g
    step = m * lax.rsqrt(v + 1e-8) + 0.1 * w
    return (w - 0.02 * step).astype(BF), m, v


def solution(mesh):
    def step(x, dy, *arrays):
        weights, m, v = (arrays[i : i + 3] for i in (0, 3, 6))
        *grads, factor = gradients(x[0], dy[0], *weights)
        new = [adamw(up(w), m, v, up(g) * factor[0, 0]) for w, m, v, g in zip(weights, m, v, grads, strict=True)]
        return tuple(one[which] for which in THREE for one in new)

    states, cut = P(("rep", "r", "s"), None, None), P(None, "s", None)
    return jax.shard_map(
        step,
        mesh=mesh,
        in_specs=(states, states) + (cut,) * 9,
        out_specs=(P("rep", "s", None),) * 9,
        check_vma=False,
    )
```

```python
import functools

import jax
import jax.numpy as jnp
from jax import lax
from jax.experimental import pallas as pl
from jax.experimental.pallas import tpu as pltpu
from jax.sharding import PartitionSpec as P

MESH = pl.DeviceIdType.MESH
BF, F32 = jnp.bfloat16, jnp.float32
ANY = pl.BlockSpec(memory_space=pl.ANY)
NN = (((1,), (0,)), ((), ()))
NT = (((1,), (1,)), ((), ()))
TN = (((0,), (0,)), ((), ()))
PAIR, THREE = range(2), range(3)
N, D, FF = 4096, 1024, 2816
STRIP, PART = 128, 64
C = 2 * STRIP
NC = FF // C
R = 512
T = 2 * R
TRIPS, TILES = N // T, N // R
WIDE = 4
LONG = WIDE * R
HALF = D // 2
ROWS, PB = 16, 32
EPS = 1e-6
EARLY, AT = 4, 13


def dot(a, b, how):
    return lax.dot_general(a, b, how, preferred_element_type=F32)


def ds(start, size):
    return pl.ds(pl.multiple_of(start, size), size)


def up(v):
    return v.astype(F32)


def odd(v):
    return lax.rem(v, 2)


def loop(first, last, body):
    def step(i, nothing):
        body(i)
        return nothing

    lax.fori_loop(first, last, step, 0)


def passes(count, prepare, finish, unroll):
    def step(i):
        parts = [ds((i * unroll + k) * ROWS, ROWS) for k in range(unroll)]
        ready = [prepare(rows) for rows in parts]
        for rows, value in zip(parts, ready):
            finish(rows, value)

    loop(0, count // (ROWS * unroll), step)


def before(j, u, count):
    return jnp.where(j == 0, count - 1, j - 1), jnp.where(j == 0, u - 1, u)


def scale_of(wide):
    return lax.rsqrt(jnp.mean(wide * wide, -1, keepdims=True) + EPS)


class Gather:
    def __init__(self, layer, shards, gu, wd, sems, sends, halves):
        self.layer, self.shards, self.gu, self.wd, self.halves = layer, shards, gu, wd, halves
        self.sems, self.sends = sems, sends
        self.me, self.y = lax.axis_index("s"), lax.axis_index("r")
        self.x, self.c = self.me // 2, odd(self.me)
        self.sib, self.xn = self.me + 1 - 2 * self.c, lax.rem(self.me + 2, 4)
        self.diagonal = self.xn + 1 - 2 * self.c
        self.peers = {"sib": {"s": self.sib}, "xn": {"s": self.xn}, "yn": {"r": 1 - self.y}, "diagonal": {"s": self.diagonal}}
        self.whole = (0, C)

    def far(self, src, dst, kind, where, which):
        row = kind % 5
        sem = self.sems[kind // 5].at[row if self.halves else (row + 1) // 2, where]
        return pltpu.make_async_remote_copy(src, dst, self.sends.at[kind], sem, device_id=self.peers[which], device_id_type=MESH)

    def strips(self, p, part):
        start, size = part
        for m in PAIR:
            for k in PAIR:
                yield (self.shards[m].at[self.layer, ds(start, size), ds((p + NC * k) * STRIP, STRIP)],
                       self.gu.at[p, m, ds(C * self.me + start, size), pl.ds(STRIP * k, STRIP)])

    def block(self, p, owner, part):
        start, size = part
        return self.gu.at[p, :, ds(C * owner + start, size), :]

    def owner(self, p, i):
        return (2 * p + i) // NC

    def shard_rows(self, p, i):
        return self.shards[2].at[self.layer, ds((2 * p + i - NC * self.c) * PART, PART), :]

    def rows(self, p, i, x, half=None):
        rows = ds(STRIP * x + PART * i, PART)
        return self.wd.at[p, rows, :] if half is None else self.wd.at[p, rows, ds(HALF * half, HALF)]

    def mine(self, p, i, yes, no=None):
        pl.when(self.owner(p, i) == self.c)(yes)
        if no is not None:
            pl.when(self.owner(p, i) != self.c)(no)

    def part(self, h):
        return (STRIP * h, STRIP) if self.halves else self.whole

    def half(self, h):
        return h if self.halves else None

    def issue(self, p):
        for src, dst in self.strips(p, self.part(self.y)):
            self.far(src, dst, 1, p, "xn").start()
        for i in PAIR:
            def send(i=i):
                src = self.shard_rows(p, i)
                if self.halves:
                    src = src.at[:, ds(HALF * self.y, HALF)]
                self.far(src, self.rows(p, i, self.x, self.half(self.y)), 6, 2 * p + i, "xn").start()
            self.mine(p, i, send)

    def issue_near(self, p):
        for src, dst in self.strips(p, self.whole):
            self.far(src, dst, 0, p, "sib").start()
        for i in PAIR:
            def send(i=i):
                self.far(self.shard_rows(p, i), self.rows(p, i, self.x), 5, 2 * p + i, "sib").start()
            self.mine(p, i, send)

    def pass_on(self, p):
        block = self.block(p, self.xn, self.part(self.y))
        self.far(block, block, 1, p, "xn").wait_recv()
        if self.halves:
            self.far(block, block, 2, p, "yn").start()
        self.far(block, block, 3, p, "sib").start()
        for i in PAIR:
            def send(i=i):
                rows = self.rows(p, i, 1 - self.x, self.half(self.y))
                self.far(rows, rows, 6, 2 * p + i, "xn").wait_recv()
                if self.halves:
                    self.far(rows, rows, 7, 2 * p + i, "yn").start()
                self.far(rows, rows, 8, 2 * p + i, "sib").start()
            self.mine(p, i, send)

    def pass_on_y(self, p):
        block = self.block(p, self.xn, self.part(1 - self.y))
        self.far(block, block, 2, p, "yn").wait_recv()
        self.far(block, block, 4, p, "sib").start()
        for i in PAIR:
            def send(i=i):
                rows = self.rows(p, i, 1 - self.x, 1 - self.y)
                self.far(rows, rows, 7, 2 * p + i, "yn").wait_recv()
                self.far(rows, rows, 9, 2 * p + i, "sib").start()
            self.mine(p, i, send)

    def arrived(self, p):
        block = self.block(p, self.sib, self.whole)
        self.far(block, block, 0, p, "sib").wait_recv()
        ways = ((3, 8, self.y), (4, 9, 1 - self.y)) if self.halves else ((3, 8, self.y),)
        for kind, _, h in ways:
            block = self.block(p, self.diagonal, self.part(h))
            self.far(block, block, kind, p, "sib").wait_recv()
        for i in PAIR:
            def wait(i=i):
                rows = self.rows(p, i, self.x)
                self.far(rows, rows, 5, 2 * p + i, "sib").wait_recv()
                for _, kind, h in ways:
                    rows = self.rows(p, i, 1 - self.x, self.half(h))
                    self.far(rows, rows, kind, 2 * p + i, "sib").wait_recv()
            pl.when(self.owner(p, i) != self.c)(wait)

    def finish(self):
        for kind in (range(10) if self.halves else (0, 1, 3, 5, 6, 8)):
            all_rows = kind in (0, 5) or not self.halves
            if kind < 5:
                block = self.gu.at[:, :, pl.ds(0, C if all_rows else STRIP), :]
            else:
                block = self.wd.at[:, pl.ds(0, PART), :] if all_rows else self.wd.at[:, pl.ds(0, PART), pl.ds(0, HALF)]
            self.far(block, block, kind, 0, "sib").wait_send()


def kernel(x_hbm, dy_hbm, w_gate, w_up, w_down,
           h_hbm, a0_hbm, gate_hbm, up_hbm, wd0_hbm, gu1_hbm, wd1_hbm, gg_hbm, gu_hbm, gd_hbm, factor_ref,
           a, da, sq, sqs,
           isem, osem, tsem, wsem, xsem, own, gsem0, dsem0, sends0, gsem1, dsem1, sends1, outs_sem, dsem, ra, rb, rc, sa, sb, sc, fsem, inside):
    shards = (w_gate, w_up, w_down)
    g1 = Gather(1, shards, gu1_hbm, wd1_hbm, (gsem1, dsem1), sends1, False)
    me, x, c, peers = g1.me, g1.x, g1.c, g1.peers

    def move(src, dst, sem):
        return pltpu.make_async_copy(src, dst, sem)

    def first_layer(gu, wd, xt, gt, ut, *act):
        g0 = Gather(0, shards, gu, wd, (gsem0, dsem0), sends0, True)

        def saves(p, t, slot):
            return [move(src.at[slot], dst.at[p, ds(t * LONG, LONG)], osem.at[slot, i]) for i, (src, dst) in enumerate(((gt, gate_hbm), (ut, up_hbm)))]

        def local(p, wait):
            if wait:
                block = g0.block(p, me, g0.whole)
                move(block, block, own.at[p, 2]).wait()
            else:
                for src, dst in g0.strips(p, g0.whole):
                    move(src, dst, own.at[p, 2]).start()
            for i in PAIR:
                def go(i=i):
                    copy = move(g0.shard_rows(p, i), g0.rows(p, i, x), own.at[p, i])
                    copy.wait() if wait else copy.start()
                g0.mine(p, i, go)

        def keep(p):
            return move(wd.at[p], wd0_hbm.at[p], fsem.at[3])

        xin = [move(x_hbm.at[pl.ds(t * T, T)], a.at[t], isem.at[0, t]) for t in range(TRIPS)]
        turned = [move(xt.at[odd_], a0_hbm.at[t, :, pl.ds(R * odd_, R)], isem.at[1, 2 * t + odd_]) for t in range(TRIPS) for odd_ in PAIR]
        for copy in xin:
            copy.start()
        barrier = pltpu.get_barrier_semaphore()
        for peer in peers.values():
            pl.semaphore_signal(barrier, inc=1, device_id=peer, device_id_type=MESH)
        pl.semaphore_wait(barrier, len(peers))

        def issue0(p):
            g0.issue(p)

            @pl.when(p < 2)
            def _():
                g0.issue_near(p)

            local(p, False)

        def issue1(p):
            g1.issue(p)

        loop(0, 2, issue0)
        for t in range(TRIPS):
            xin[t].wait()

            def put(rows, scale):
                a[t, rows, :] = (up(a[t, rows, :]) * scale).astype(BF)

            passes(T, lambda rows: scale_of(up(a[t, rows, :])), put, 8)
            for h in PAIR:
                if t >= 1:
                    turned[2 * t + h - 2].wait()
                for k in PAIR:
                    xt[h, :, C * k : C * (k + 1)] = a[t, R * h + C * k : R * h + C * (k + 1), :].T
                turned[2 * t + h].start()
            if t == 0:
                loop(2, NC, issue0)
            if t == 1:
                g0.pass_on(0)
            if t == 2:
                g0.pass_on(1)
                loop(0, NC, issue1)
        g0.pass_on_y(0)

        def down(i, j, p):
            rows = ds(j * R, R)
            da[rows, :] = jnp.where(p == 0, 0.0, da[rows, :]) + dot(act[i][...], wd[jnp.maximum(p, 0)], NN)

        def chunk(p):
            def trip(t):
                now = 2 * p + t

                @pl.when((now >= 1) & (now + 1 < NC))
                def _():
                    g0.pass_on(now + 1)

                @pl.when((now == 1) | (now >= 3) & (now <= NC))
                def _():
                    g0.pass_on_y(jnp.maximum(now - 1, 1))

                @pl.when(now + 2 < NC)
                def _():
                    g0.issue_near(now + 2)

                @pl.when(now >= NC)
                def _():
                    g1.issue_near(now - NC)

                early = (2 * (now - AT) + 4) // 5

                @pl.when((now >= AT) & ((5 * early) // 2 == now - AT) & (early < EARLY))
                def _():
                    g1.pass_on(early)

                @pl.when(t == 0)
                def _():
                    local(p, True)
                    g0.arrived(p)
                    keep(p).start()

                @pl.when(now >= 2)
                def _():
                    for copy in saves(0, 0, t):
                        copy.wait()

                for i in range(WIDE):
                    part, j = pl.ds(i * R, R), WIDE * t + i
                    at = a[2 * t + i // 2, i % 2 * R : (i % 2 + 1) * R, :]
                    gt[t, part] = dot(at, gu[p, 0], NN)
                    ut[t, part] = dot(at, gu[p, 1], NN)
                    down(1 - i % 2, *before(j, p, TILES))
                    for k in range(0, R, PB):
                        g, u = gt[t, pl.ds(i * R + k, PB)], ut[t, pl.ds(i * R + k, PB)]
                        act[i % 2][k : k + PB] = (g / (1.0 + jnp.exp(-g)) * u).astype(BF)
                for copy in saves(p, t, t):
                    copy.start()

            loop(0, N // LONG, trip)

        loop(0, NC, chunk)
        down(1, TILES - 1, NC - 1)
        for copy in turned[-2:]:
            copy.wait()
        for o in PAIR:
            for copy in saves(0, 0, o):
                copy.wait()
        move(wd, wd0_hbm, fsem.at[3]).wait()
        g0.finish()

    pl.run_scoped(first_layer, pltpu.VMEM((NC, 2, D, C), BF), pltpu.VMEM((NC, C, D), BF), pltpu.VMEM((2, D, R), BF), *[pltpu.VMEM((2, LONG, C), F32)] * 2, *[pltpu.VMEM((R, C), BF)] * 2)

    def rest(dy, wd, acc_g, acc_u, acc_d, send_a, recv_a, own_b, send_b, recv_b, send_c, recv_c, out_gu, out_d):
        def copy_a(u, m):
            return pltpu.make_async_remote_copy(send_a.at[m], recv_a.at[odd(u), m], sa.at[m], ra.at[odd(u), m], device_id=peers["sib"], device_id_type=MESH)

        def copy_b(u, m):
            s, q = odd(u), lax.rem(u, 4)
            return pltpu.make_async_remote_copy(send_b.at[s, m], recv_b.at[q, m], sb.at[s, m], rb.at[q, m], device_id=peers["xn"], device_id_type=MESH)

        def copy_c(u, m):
            s, q = odd(u), lax.rem(u, 4)
            return pltpu.make_async_remote_copy(send_c.at[s, m], recv_c.at[q, m], sc.at[s, m], rc.at[q, m], device_id=peers["yn"], device_id_type=MESH)

        def free(copy, u, least):
            @pl.when(u >= least)
            def _():
                for m in THREE:
                    copy(u - least, m).wait_send()

        def outs(u, m, wait):
            s, layer, p = odd(u), 1 - u // NC, lax.rem(u, NC)

            def go(copy, far=False):
                (copy.wait_send if far else copy.wait)() if wait else copy.start()

            for i in PAIR:
                sem = outs_sem.at[s, 2 * m + i]
                if m < 2:
                    go(move(out_gu.at[s, m, :, pl.ds(STRIP * i, STRIP)], (gg_hbm, gu_hbm)[m].at[layer, :, ds((p + NC * i) * STRIP, STRIP)], sem))
                    continue
                src = out_d.at[s, pl.ds(PART * i, PART), :]
                dst = gd_hbm.at[layer, ds((2 * p + i - NC * g1.owner(p, i)) * PART, PART), ds(HALF * c, HALF)]
                g1.mine(p, i, lambda: go(move(src, dst, sem)),
                        lambda: go(pltpu.make_async_remote_copy(src, dst, sem, dsem.at[layer], device_id=peers["sib"], device_id_type=MESH), True))

        def part(s, m, xd, cc):
            if m < 2:
                return [(pl.ds(0, C), (acc_g, acc_u)[m][s, ds(2 * C * xd + C * cc, C), :])]
            return [(pl.ds(STRIP * k, STRIP), acc_d[s, ds(STRIP * xd, STRIP), ds(HALF * cc + C * k, C)]) for k in PAIR]

        def stage_a(u):
            free(copy_a, u, 1)
            for m in THREE:
                for xd in PAIR:
                    for rows, term in part(odd(u), m, xd, 1 - c):
                        send_a[m, xd, rows, :] = term.astype(BF)
                copy_a(u, m).start()

        def stage_b(u):
            s = odd(u)
            free(copy_b, u, 2)
            for m in THREE:
                copy_a(u, m).wait_recv()
                for rows, term in part(s, m, 1 - x, c):
                    send_b[s, m, rows, :] = (term + up(recv_a[s, m, 1 - x, rows, :])).astype(BF)
                copy_b(u, m).start()
            for m in THREE:
                for rows, term in part(s, m, x, c):
                    own_b[s, m, rows, :] = term + up(recv_a[s, m, x, rows, :])

        def stage_c(u):
            s = odd(u)
            free(copy_c, u, 2)
            for m in THREE:
                copy_b(u, m).wait_recv()
                send_c[s, m] = (own_b[s, m] + up(recv_b[lax.rem(u, 4), m])).astype(BF)
                copy_c(u, m).start()

        def stage_d(u):
            s = odd(u)

            @pl.when(u >= 2)
            def _():
                for m in THREE:
                    outs(u - 2, m, True)

            for m in THREE:
                copy_c(u, m).wait_recv()
                total = (up(send_c[s, m]) + up(recv_c[lax.rem(u, 4), m])).astype(BF)
                if m < 2:
                    out_gu[s, m] = total
                else:
                    for k in PAIR:
                        out_d[s, :, C * k : C * (k + 1)] = total[STRIP * k : STRIP * (k + 1)]
                sq[m] += jnp.sum((up(total) * up(total)).reshape(C // 8, 8, C), axis=0)
                outs(u, m, False)

        def travel(u, event, when):
            for stage, lag in (((stage_c, 3),), ((stage_a, 1), (stage_d, 4)), ((stage_b, 1),))[event]:
                @pl.when(when & (u >= lag))
                def _():
                    stage(u - lag)

        def load0(p, slot):
            return move(wd0_hbm.at[p], wd.at[slot], wsem.at[slot, 10])

        def saved(p, t):
            return [move(src.at[p, ds(t * LONG, LONG)], da.at[ds(t * LONG, LONG), pl.ds(C * i, C)], tsem.at[t, i]) for i, src in enumerate((gate_hbm, up_hbm))]

        def dyin(t):
            return move(dy_hbm.at[ds(t * T, T)], dy.at[ds(t * T, T)], isem.at[0, t])

        def new(t):
            return move(a0_hbm.at[t], a.at[t], isem.at[1, t])

        def arithmetic(rows, dt, act, dg, du):
            def pointwise(block, i, gate_and_up):
                for k in range(0, R, PB):
                    (g, u), d, there = gate_and_up(k), up(dt[odd_of(block, i), k : k + PB].astype(BF)), slice(R * i + k, R * i + k + PB)
                    sig = 1.0 / (1.0 + jnp.exp(-g))
                    silu = g * sig
                    act[block][there] = (silu * u).astype(BF)
                    du[block][there] = (d * silu).astype(BF)
                    dg[block][there] = (d * u * (sig + silu * (1.0 - sig))).astype(BF)

            def odd_of(block, i):
                return i if rows == T else block

            def weight_grads(block, k, u, turned=False, row=None):
                s, n = odd(u + 2), k if row is None else row
                dyt = dy[ds(n * rows, rows), :]
                at, how = (a[n], NN) if turned else (a[n // 2, R * block : R * (block + 1), :], TN)
                acc_g[s] = jnp.where(k == 0, 0.0, acc_g[s]) + dot(at, dg[block][...], how)
                acc_u[s] = jnp.where(k == 0, 0.0, acc_u[s]) + dot(at, du[block][...], how)
                acc_d[s] = jnp.where(k == 0, 0.0, acc_d[s]) + dot(act[block][...], dyt, TN)

            return pointwise, weight_grads

        def last_layer(wgu, gt, ut, dt, act0, act1, dg0, dg1, du0, du1, ht):
            dg, du = (dg0, dg1), (du0, du1)
            pointwise, weight_grads = arithmetic(R, dt, (act0, act1), dg, du)

            def loads(p, slot, wait):
                def go(src, dst, k):
                    copy = move(src, dst, wsem.at[slot, k])
                    copy.wait() if wait else copy.start()

                for m in PAIR:
                    for k in PAIR:
                        go(shards[m].at[1, :, ds((p + NC * k) * STRIP, STRIP)], wgu.at[slot, m, ds(C * me, C), pl.ds(STRIP * k, STRIP)], 2 * m + k)
                for k, owner in enumerate((g1.sib, g1.xn, g1.diagonal)):
                    go(g1.block(p, owner, g1.whole), wgu.at[slot, :, ds(C * owner, C), :], 4 + k)
                for i in PAIR:
                    there = wd.at[slot, ds(STRIP * x + PART * i, PART), :]
                    g1.mine(p, i, lambda: go(g1.shard_rows(p, i), there, 7 + i), lambda: go(g1.rows(p, i, x), there, 7 + i))
                go(wd1_hbm.at[p, ds(STRIP * (1 - x), STRIP), :], wd.at[slot, ds(STRIP * (1 - x), STRIP), :], 9)

            def tile(hbm, j, back=False):
                k = lax.rem(j, 4)
                there, here = hbm.at[ds(j * R, R)], ht.at[k]
                return move(here, there, xsem.at[1, k]) if back else move(there, here, xsem.at[0, k])

            neighbours = ("sib", "xn", "yn")
            for which in neighbours:
                pl.semaphore_signal(inside, inc=1, device_id=peers[which], device_id_type=MESH)
            for j in range(4):
                tile(x_hbm, j).start()
            g1.arrived(0)
            loads(0, 0, False)
            for t in range(TRIPS):
                dyin(t).start()
            sq[...] = jnp.zeros_like(sq)

            def output(j):
                tile(x_hbm, j).wait()
                k, t, h = lax.rem(j, 4), j // 2, odd(j)

                def sums(rows):
                    value = (up(ht[k, rows, :]) + up(da[ds(j * R + rows.start, ROWS), :].astype(BF))).astype(BF)
                    ht[k, rows, :] = value
                    return scale_of(up(value))

                def put(rows, scale):
                    a[t, ds(h * R + rows.start, ROWS), :] = (up(ht[k, rows, :]) * scale).astype(BF)

                passes(R, sums, put, 8)
                tile(h_hbm, j, True).start()

            def norm_back(j):
                tile(h_hbm, j).wait()
                k = lax.rem(j, 4)

                def parts(part):
                    rows = ds(j * R + part.start, ROWS)
                    return rows, up(ht[k, part, :]), up(da[rows, :].astype(BF))

                def sums(part):
                    _, wide, g = parts(part)
                    scale = scale_of(wide)
                    return scale, jnp.sum(g * wide, -1, keepdims=True) * (scale * scale * scale * (1.0 / D))

                def put(part, value):
                    rows, wide, g = parts(part)
                    scale, inner = value
                    dy[rows, :] = (up(dy[rows, :]) + up((g * scale - wide * inner).astype(BF))).astype(BF)

                passes(R, sums, put, 4)

                @pl.when(odd(j) == 1)
                def _():
                    new(j // 2).start()

                @pl.when(j + 4 < TILES)
                def _():
                    tile(h_hbm, j + 4).start()

            def input_grads(i, j, u, row=None):
                w, rows = odd(u + 2), ds((j if row is None else row) * R, R)
                da[rows, :] = jnp.where(u == 0, 0.0, da[rows, :]) + dot(dg[i][...], wgu[w, 0], NT) + dot(du[i][...], wgu[w, 1], NT)

            def chunk1(u):
                w = odd(u)
                loads(u, w, True)

                @pl.when(u == NC - 1)
                def _():
                    for j in range(4):
                        tile(h_hbm, j).start()

                def trip(t):
                    now = 2 * u + t
                    first, last = u == 0, u == NC - 1
                    travel(u, 0, t == 0)
                    travel(u, 1, t == 1)

                    @pl.when(first)
                    def _():
                        for i in range(WIDE):
                            output(WIDE * t + i)
                        for i in PAIR:
                            dyin(2 * t + i).wait()

                    @pl.when(now == 2)
                    def _():
                        pl.semaphore_wait(inside, len(neighbours))
                        for j in range(TILES - WIDE, TILES):
                            tile(h_hbm, j, True).wait()

                    @pl.when(EARLY + now < NC)
                    def _():
                        g1.pass_on(EARLY + now)

                    @pl.when((t == 1) & (u + 1 < NC))
                    def _():
                        g1.arrived(u + 1)
                        loads(u + 1, 1 - w, False)

                    @pl.when((t == 1) & last)
                    def _():
                        load0(0, 1 - w).start()
                        for j in range(WIDE - 1):
                            norm_back(j)

                    for i in range(WIDE):
                        j, b, part = WIDE * t + i, i % 2, slice(i % 2 * R, (i % 2 + 1) * R)
                        at, dyt = a[2 * t + i // 2, part, :], dy[ds(j * R, R), :]
                        gt[b] = dot(at, wgu[w, 0], NN)
                        ut[b] = dot(at, wgu[w, 1], NN)
                        dt[b] = dot(dyt, wd[w], NT)
                        pj, pu = before(j, u, TILES)
                        row = jnp.where((now == 0) & (i == 0), 1 - b, pj)
                        input_grads(1 - b, pj, pu, row)
                        weight_grads(1 - b, pj, pu, False, row)
                        pointwise(b, 0, lambda k: (gt[b, k : k + PB], ut[b, k : k + PB]))

                    @pl.when(now == 0)
                    def _():
                        for j in range(WIDE):
                            tile(h_hbm, j, True).wait()
                            tile(x_hbm, j + WIDE).start()

                    travel(u, 2, t == 1)

                loop(0, N // LONG, trip)

            loop(0, NC, chunk1)
            input_grads(1, TILES - 1, NC - 1)
            weight_grads(1, TILES - 1, NC - 1)
            norm_back(WIDE - 1)
            for copy in saved(0, 0):
                copy.start()
            for j in range(WIDE, TILES):
                norm_back(j)

        def first_backward(dt, act0, act1, dg0, dg1, du0, du1):
            pointwise, weight_grads = arithmetic(T, dt, (act0, act1), (dg0, dg1), (du0, du1))
            for ref in (act1, dg1, du1):
                ref[...] = jnp.zeros_like(ref)

            def chunk0(u):
                w, p = odd(u), u - NC
                load0(p, w).wait()

                @pl.when(p + 1 < NC)
                def _():
                    load0(p + 1, 1 - w).start()

                def trip(t):
                    travel(u, 0, t == 0)
                    travel(u, 1, t == 1)

                    @pl.when(p == 0)
                    def _():
                        for i in PAIR:
                            new(2 * t + i).wait()

                    for copy in saved(p, t):
                        copy.wait()

                    @pl.when((t == 0) | (p + 1 < NC))
                    def _():
                        for copy in saved(p + t, 1 - t):
                            copy.start()

                    for block in PAIR:
                        k = 2 * t + block
                        for i in PAIR:
                            dt[i] = dot(dy[ds(k * T + i * R, R), :], wd[w], NT)
                            if i == 0:
                                pk, pu = before(k, u, TRIPS)
                                weight_grads(1 - block, pk, pu, True, jnp.where((p == 0) & (k == 0), 0, pk))

                            def gate_and_up(part):
                                rows = ds(k * T + i * R + part, PB)
                                return da[rows, :C], da[rows, C : 2 * C]

                            pointwise(block, i, gate_and_up)

                    travel(u, 2, t == 1)

                loop(0, N // LONG, trip)

            loop(NC, 2 * NC, chunk0)
            weight_grads(1, TRIPS - 1, 2 * NC - 1, True)

        f, third = pltpu.VMEM, pltpu.VMEM((2, R, C), F32)
        pl.run_scoped(last_layer, f((2, 2, D, C), BF), *[third] * 3, *[f((R, C), BF)] * 6, f((4, R, D), BF))
        pl.run_scoped(first_backward, third, *[f((T, C), BF)] * 6)

        L = 2 * NC - 1
        for stage, u in ((stage_a, L), (stage_c, L - 2), (stage_d, L - 3), (stage_b, L), (stage_c, L - 1), (stage_d, L - 2), (stage_c, L), (stage_d, L - 1), (stage_d, L)):
            stage(u)
        free(copy_a, L, 0)
        for u in (L - 1, L):
            free(copy_b, u, 0)
            free(copy_c, u, 0)
        squares = sq[0] + sq[1] + sq[2]
        sqs[me] = squares[:, :STRIP] + squares[:, STRIP:]
        others = [pltpu.make_async_remote_copy(sqs.at[me], sqs.at[me], fsem.at[k], dsem.at[2 + k], device_id=peers[which], device_id_type=MESH)
                  for k, which in enumerate(("sib", "xn", "diagonal"))]
        for copy in others:
            copy.start()
        g1.finish()
        for copy in others:
            copy.wait()
        mean = jnp.sum(sqs[...]) / (3.0 * 2 * D * FF)
        factor_ref[...] = jnp.full(factor_ref.shape, 1.0) * jnp.minimum(1.0, 0.5 * lax.rsqrt(jnp.full(factor_ref.shape, mean) + 1e-30))
        for m in THREE:
            outs(L - 1, m, True)
            outs(L, m, True)
        for layer in PAIR:
            got = gd_hbm.at[layer, :, ds(HALF * (1 - c), HALF)]
            move(got, got, dsem.at[layer]).wait()

    piece, f = (3, C, C), pltpu.VMEM
    pl.run_scoped(
        rest,
        f((N, D), BF), f((2, C, D), BF), f((2, D, C), F32), f((2, D, C), F32), f((2, C, D), F32),
        f((3, 2, C, C), BF), f((2, 3, 2, C, C), BF), f((2,) + piece, F32),
        f((2,) + piece, BF), f((4,) + piece, BF), f((2,) + piece, BF), f((4,) + piece, BF), f((2, 2, C, C), BF), f((2, STRIP, HALF), BF),
    )


def gradients(x, dy, *shards):
    dma, shape = pltpu.SemaphoreType.DMA, jax.ShapeDtypeStruct
    sides = [[dma((kinds, NC)), dma((kinds, 2 * NC)), dma((10,))] for kinds in (5, 3)]
    return pl.pallas_call(
        kernel,
        name="gradients",
        in_specs=[ANY] * 5,
        out_specs=[ANY] * 10 + [pl.BlockSpec(memory_space=pltpu.VMEM)],
        out_shape=[shape((N, D), BF), shape((TRIPS, D, T), BF), shape((NC, N, C), F32), shape((NC, N, C), F32),
                   shape((NC, C, D), BF), shape((NC, 2, D, C), BF), shape((NC, C, D), BF),
                   shape((2, C, FF), BF), shape((2, C, FF), BF), shape((2, FF // 4, D), BF), shape((8, STRIP), F32)],
        scratch_shapes=[
            pltpu.VMEM((TRIPS, T, D), BF), pltpu.VMEM((N, D), F32),
            pltpu.VMEM((3, 8, C), F32), pltpu.VMEM((4, 8, STRIP), F32),
            dma((2, TILES)), *[dma((2, 2))] * 2, dma((2, 11)), dma((2, 4)), dma((NC, 3)), *sides[0], *sides[1], dma((2, 6)), dma((5,)),
            dma((2, 3)), dma((4, 3)), dma((4, 3)), dma((3,)), dma((2, 3)), dma((2, 3)), dma((4,)), pltpu.SemaphoreType.REGULAR,
        ],
        compiler_params=pltpu.CompilerParams(vmem_limit_bytes=67_000_000, collective_id=0, has_side_effects=True),
    )(x, dy, *shards)[-4:]


def adamw(w, m, v, g):
    m = 0.9 * m + 0.1 * g
    v = 0.95 * v + 0.05 * g * g
    step = m * lax.rsqrt(v + 1e-8) + 0.1 * w
    return (w - 0.02 * step).astype(BF), m, v


def solution(mesh):
    def step(x, dy, *arrays):
        weights, m, v = (arrays[i : i + 3] for i in (0, 3, 6))
        *grads, factor = gradients(x[0], dy[0], *weights)
        new = [adamw(up(w), m, v, up(g) * factor[0, 0]) for w, m, v, g in zip(weights, m, v, grads, strict=True)]
        return tuple(one[which] for which in THREE for one in new)

    states, cut = P(("rep", "r", "s"), None, None), P(None, "s", None)
    return jax.shard_map(
        step,
        mesh=mesh,
        in_specs=(states, states) + (cut,) * 9,
        out_specs=(P("rep", "s", None),) * 9,
        check_vma=False,
    )
```

```python
import functools

import jax
import jax.numpy as jnp
from jax import lax
from jax.experimental import pallas as pl
from jax.experimental.pallas import tpu as pltpu
from jax.sharding import PartitionSpec as P

MESH = pl.DeviceIdType.MESH
BF, F32 = jnp.bfloat16, jnp.float32
ANY = pl.BlockSpec(memory_space=pl.ANY)
NN = (((1,), (0,)), ((), ()))
NT = (((1,), (1,)), ((), ()))
TN = (((0,), (0,)), ((), ()))
PAIR, THREE = range(2), range(3)
N, D, FF = 4096, 1024, 2816
STRIP, PART = 128, 64
C = 2 * STRIP
NC = FF // C
R = 512
T = 2 * R
TRIPS, TILES = N // T, N // R
WIDE = 4
LONG = WIDE * R
HALF = D // 2
ROWS, PB = 16, 32
EPS = 1e-6
EARLY, AT = 4, 13


def dot(a, b, how):
    return lax.dot_general(a, b, how, preferred_element_type=F32)


def ds(start, size):
    return pl.ds(pl.multiple_of(start, size), size)


def up(v):
    return v.astype(F32)


def odd(v):
    return lax.rem(v, 2)


def loop(first, last, body):
    def step(i, nothing):
        body(i)
        return nothing

    lax.fori_loop(first, last, step, 0)


def passes(count, prepare, finish, unroll):
    def step(i):
        parts = [ds((i * unroll + k) * ROWS, ROWS) for k in range(unroll)]
        ready = [prepare(rows) for rows in parts]
        for rows, value in zip(parts, ready):
            finish(rows, value)

    loop(0, count // (ROWS * unroll), step)


def before(j, u, count):
    return jnp.where(j == 0, count - 1, j - 1), jnp.where(j == 0, u - 1, u)


def scale_of(wide):
    return lax.rsqrt(jnp.mean(wide * wide, -1, keepdims=True) + EPS)


class Gather:
    def __init__(self, layer, shards, gu, wd, sems, sends, halves):
        self.layer, self.shards, self.gu, self.wd, self.halves = layer, shards, gu, wd, halves
        self.sems, self.sends = sems, sends
        self.me, self.y = lax.axis_index("s"), lax.axis_index("r")
        self.x, self.c = self.me // 2, odd(self.me)
        self.sib, self.xn = self.me + 1 - 2 * self.c, lax.rem(self.me + 2, 4)
        self.diagonal = self.xn + 1 - 2 * self.c
        self.peers = {"sib": {"s": self.sib}, "xn": {"s": self.xn}, "yn": {"r": 1 - self.y}, "diagonal": {"s": self.diagonal}}
        self.whole = (0, C)

    def far(self, src, dst, kind, where, which):
        row = kind % 5
        sem = self.sems[kind // 5].at[row if row < 3 else 0, where]
        return pltpu.make_async_remote_copy(src, dst, self.sends.at[kind], sem, device_id=self.peers[which], device_id_type=MESH)

    def strips(self, p, part):
        start, size = part
        for m in PAIR:
            for k in PAIR:
                yield (self.shards[m].at[self.layer, ds(start, size), ds((p + NC * k) * STRIP, STRIP)],
                       self.gu.at[p, m, ds(C * self.me + start, size), pl.ds(STRIP * k, STRIP)])

    def block(self, p, owner, part):
        start, size = part
        return self.gu.at[p, :, ds(C * owner + start, size), :]

    def owner(self, p, i):
        return (2 * p + i) // NC

    def shard_rows(self, p, i):
        return self.shards[2].at[self.layer, ds((2 * p + i - NC * self.c) * PART, PART), :]

    def rows(self, p, i, x, half=None):
        rows = ds(STRIP * x + PART * i, PART)
        return self.wd.at[p, rows, :] if half is None else self.wd.at[p, rows, ds(HALF * half, HALF)]

    def mine(self, p, i, yes, no=None):
        pl.when(self.owner(p, i) == self.c)(yes)
        if no is not None:
            pl.when(self.owner(p, i) != self.c)(no)

    def part(self, h):
        return (STRIP * h, STRIP) if self.halves else self.whole

    def half(self, h):
        return h if self.halves else None

    def issue(self, p):
        for src, dst in self.strips(p, self.part(self.y)):
            self.far(src, dst, 1, p, "xn").start()
        for i in PAIR:
            def send(i=i):
                src = self.shard_rows(p, i)
                if self.halves:
                    src = src.at[:, ds(HALF * self.y, HALF)]
                self.far(src, self.rows(p, i, self.x, self.half(self.y)), 6, 2 * p + i, "xn").start()
            self.mine(p, i, send)

    def issue_near(self, p):
        for src, dst in self.strips(p, self.whole):
            self.far(src, dst, 0, p, "sib").start()
        for i in PAIR:
            def send(i=i):
                self.far(self.shard_rows(p, i), self.rows(p, i, self.x), 5, 2 * p + i, "sib").start()
            self.mine(p, i, send)

    def pass_on(self, p):
        block = self.block(p, self.xn, self.part(self.y))
        self.far(block, block, 1, p, "xn").wait_recv()
        if self.halves:
            self.far(block, block, 2, p, "yn").start()
        self.far(block, block, 3, p, "sib").start()
        for i in PAIR:
            def send(i=i):
                rows = self.rows(p, i, 1 - self.x, self.half(self.y))
                self.far(rows, rows, 6, 2 * p + i, "xn").wait_recv()
                if self.halves:
                    self.far(rows, rows, 7, 2 * p + i, "yn").start()
                self.far(rows, rows, 8, 2 * p + i, "sib").start()
            self.mine(p, i, send)

    def pass_on_y(self, p):
        block = self.block(p, self.xn, self.part(1 - self.y))
        self.far(block, block, 2, p, "yn").wait_recv()
        self.far(block, block, 4, p, "sib").start()
        for i in PAIR:
            def send(i=i):
                rows = self.rows(p, i, 1 - self.x, 1 - self.y)
                self.far(rows, rows, 7, 2 * p + i, "yn").wait_recv()
                self.far(rows, rows, 9, 2 * p + i, "sib").start()
            self.mine(p, i, send)

    def arrived(self, p):
        block = self.gu.at[p, :, pl.ds(0, 2 * C), :]
        self.far(block, block, 0, p, "sib").wait_recv()
        for i in PAIR:
            def wait(i=i):
                rows = self.wd.at[p, pl.ds(0, STRIP), :]
                self.far(rows, rows, 5, 2 * p + i, "sib").wait_recv()
            pl.when(self.owner(p, i) != self.c)(wait)

    def finish(self):
        for kind in (range(10) if self.halves else (0, 1, 3, 5, 6, 8)):
            all_rows = kind in (0, 5) or not self.halves
            if kind < 5:
                block = self.gu.at[:, :, pl.ds(0, C if all_rows else STRIP), :]
            else:
                block = self.wd.at[:, pl.ds(0, PART), :] if all_rows else self.wd.at[:, pl.ds(0, PART), pl.ds(0, HALF)]
            self.far(block, block, kind, 0, "sib").wait_send()


def kernel(x_hbm, dy_hbm, w_gate, w_up, w_down,
           h_hbm, a0_hbm, gate_hbm, up_hbm, wd0_hbm, gu1_hbm, wd1_hbm, gg_hbm, gu_hbm, gd_hbm, factor_ref,
           a, da, ht, sq, sqs,
           isem, osem, tsem, wsem, xsem, own, gsem0, dsem0, sends0, gsem1, dsem1, sends1, outs_sem, dsem, ra, rb, rc, sa, sb, sc, fsem, inside):
    shards = (w_gate, w_up, w_down)
    g1 = Gather(1, shards, gu1_hbm, wd1_hbm, (gsem1, dsem1), sends1, False)
    me, x, c, peers = g1.me, g1.x, g1.c, g1.peers

    def move(src, dst, sem):
        return pltpu.make_async_copy(src, dst, sem)

    def tile(hbm, j, back=False):
        k = lax.rem(j, 4)
        there, here = hbm.at[ds(j * R, R)], ht.at[k]
        return move(here, there, xsem.at[1, k]) if back else move(there, here, xsem.at[0, k])

    def first_layer(gu, wd, xt, gt, ut, *act):
        g0 = Gather(0, shards, gu, wd, (gsem0, dsem0), sends0, True)

        def saves(p, t, slot):
            return [move(src.at[slot], dst.at[p, ds(t * LONG, LONG)], osem.at[slot, i]) for i, (src, dst) in enumerate(((gt, gate_hbm), (ut, up_hbm)))]

        def local(p, wait):
            if wait:
                block = g0.block(p, me, g0.whole)
                move(block, block, own.at[p, 2]).wait()
            else:
                for src, dst in g0.strips(p, g0.whole):
                    move(src, dst, own.at[p, 2]).start()
            for i in PAIR:
                def go(i=i):
                    copy = move(g0.shard_rows(p, i), g0.rows(p, i, x), own.at[p, i])
                    copy.wait() if wait else copy.start()
                g0.mine(p, i, go)

        def keep(p):
            return move(wd.at[p], wd0_hbm.at[p], fsem.at[3])

        xin = [move(x_hbm.at[pl.ds(t * T, T)], a.at[t], isem.at[0, t]) for t in range(TRIPS)]
        turned = [move(xt.at[odd_], a0_hbm.at[t, :, pl.ds(R * odd_, R)], isem.at[1, 2 * t + odd_]) for t in range(TRIPS) for odd_ in PAIR]
        for copy in xin:
            copy.start()
        barrier = pltpu.get_barrier_semaphore()
        for peer in peers.values():
            pl.semaphore_signal(barrier, inc=1, device_id=peer, device_id_type=MESH)
        pl.semaphore_wait(barrier, len(peers))

        def issue0(p):
            g0.issue(p)

            @pl.when(p < 2)
            def _():
                g0.issue_near(p)
                local(p, False)

        loop(0, 2, issue0)
        for t in range(TRIPS):
            xin[t].wait()

            def put(rows, scale):
                a[t, rows, :] = (up(a[t, rows, :]) * scale).astype(BF)

            passes(T, lambda rows: scale_of(up(a[t, rows, :])), put, 8)
            for h in PAIR:
                if t >= 1:
                    turned[2 * t + h - 2].wait()
                for k in PAIR:
                    xt[h, :, C * k : C * (k + 1)] = a[t, R * h + C * k : R * h + C * (k + 1), :].T
                turned[2 * t + h].start()
            if t == 0:
                loop(2, NC, issue0)
            if t == 1:
                g0.pass_on(0)
            if t == 2:
                g0.pass_on(1)
        g0.pass_on_y(0)

        def down(i, j, p):
            rows = ds(j * R, R)
            da[rows, :] = jnp.where(p == 0, 0.0, da[rows, :]) + dot(act[i][...], wd[jnp.maximum(p, 0)], NN)

        def chunk(p):
            def trip(t):
                now = 2 * p + t

                @pl.when((now >= 1) & (now + 1 < NC))
                def _():
                    g0.pass_on(now + 1)

                @pl.when((now == 1) | (now >= 3) & (now <= NC))
                def _():
                    g0.pass_on_y(jnp.maximum(now - 1, 1))

                @pl.when(now + 2 < NC)
                def _():
                    g0.issue_near(now + 2)
                    local(now + 2, False)

                @pl.when(now < NC)
                def _():
                    g1.issue(now)

                @pl.when(now >= NC)
                def _():
                    g1.issue_near(now - NC)

                @pl.when(now == 2 * NC - 1)
                def _():
                    for j in range(WIDE):
                        tile(x_hbm, j).start()

                early = (2 * (now - AT) + 4) // 5

                @pl.when((now >= AT) & ((5 * early) // 2 == now - AT) & (early < EARLY))
                def _():
                    g1.pass_on(early)

                @pl.when(t == 0)
                def _():
                    local(p, True)
                    g0.arrived(p)
                    keep(p).start()

                @pl.when(now >= 2)
                def _():
                    for copy in saves(0, 0, t):
                        copy.wait()

                for i in range(WIDE):
                    part, j = pl.ds(i * R, R), WIDE * t + i
                    at = a[2 * t + i // 2, i % 2 * R : (i % 2 + 1) * R, :]
                    gt[t, part] = dot(at, gu[p, 0], NN)
                    ut[t, part] = dot(at, gu[p, 1], NN)
                    down(1 - i % 2, *before(j, p, TILES))
                    for k in range(0, R, PB):
                        g, u = gt[t, pl.ds(i * R + k, PB)], ut[t, pl.ds(i * R + k, PB)]
                        act[i % 2][k : k + PB] = (g / (1.0 + jnp.exp(-g)) * u).astype(BF)
                for copy in saves(p, t, t):
                    copy.start()

            loop(0, N // LONG, trip)

        loop(0, NC, chunk)
        down(1, TILES - 1, NC - 1)
        for copy in turned[-2:]:
            copy.wait()
        for o in PAIR:
            for copy in saves(0, 0, o):
                copy.wait()
        move(wd, wd0_hbm, fsem.at[3]).wait()
        g0.finish()

    pl.run_scoped(first_layer, pltpu.VMEM((NC, 2, D, C), BF), pltpu.VMEM((NC, C, D), BF), pltpu.VMEM((2, D, R), BF), *[pltpu.VMEM((2, LONG, C), F32)] * 2, *[pltpu.VMEM((R, C), BF)] * 2)

    def rest(dy, wd, acc_g, acc_u, acc_d, send_a, recv_a, own_b, send_b, recv_b, send_c, recv_c, out_gu, out_d):
        def copy_a(u, m):
            return pltpu.make_async_remote_copy(send_a.at[m], recv_a.at[odd(u), m], sa, ra.at[odd(u), m], device_id=peers["sib"], device_id_type=MESH)

        def copy_b(u, m):
            s, q = odd(u), lax.rem(u, 4)
            return pltpu.make_async_remote_copy(send_b.at[s, m], recv_b.at[q, m], sb.at[s], rb.at[q, m], device_id=peers["xn"], device_id_type=MESH)

        def copy_c(u, m):
            s, q = odd(u), lax.rem(u, 4)
            return pltpu.make_async_remote_copy(send_c.at[s, m], recv_c.at[q, m], sc.at[s], rc.at[q, m], device_id=peers["yn"], device_id_type=MESH)

        def free(ref, sem, when=True):
            pl.when(when)(lambda: move(ref, ref, sem).wait())

        def outs(u, m):
            s, layer, p = odd(u), 1 - u // NC, lax.rem(u, NC)
            sem = outs_sem.at[s]
            for i in PAIR:
                if m < 2:
                    move(out_gu.at[s, m, :, pl.ds(STRIP * i, STRIP)], (gg_hbm, gu_hbm)[m].at[layer, :, ds((p + NC * i) * STRIP, STRIP)], sem).start()
                    continue
                src = out_d.at[s, pl.ds(PART * i, PART), :]
                dst = gd_hbm.at[layer, ds((2 * p + i - NC * g1.owner(p, i)) * PART, PART), ds(HALF * c, HALF)]
                g1.mine(p, i, lambda: move(src, dst, sem).start(),
                        lambda: pltpu.make_async_remote_copy(src, dst, sem, dsem.at[layer], device_id=peers["sib"], device_id_type=MESH).start())

        def part(s, m, xd, cc):
            if m < 2:
                return [(pl.ds(0, C), (acc_g, acc_u)[m][s, ds(2 * C * xd + C * cc, C), :])]
            return [(pl.ds(STRIP * k, STRIP), acc_d[s, ds(STRIP * xd, STRIP), ds(HALF * cc + C * k, C)]) for k in PAIR]

        def stage_a(u):
            free(send_a, sa, u >= 1)
            for m in THREE:
                for xd in PAIR:
                    for rows, term in part(odd(u), m, xd, 1 - c):
                        send_a[m, xd, rows, :] = term.astype(BF)
                copy_a(u, m).start()

        def stage_b(u):
            s = odd(u)
            free(send_b.at[s], sb.at[s], u >= 2)
            for m in THREE:
                copy_a(u, m).wait_recv()
                for rows, term in part(s, m, 1 - x, c):
                    send_b[s, m, rows, :] = (term + up(recv_a[s, m, 1 - x, rows, :])).astype(BF)
                copy_b(u, m).start()
            for m in THREE:
                for rows, term in part(s, m, x, c):
                    own_b[s, m, rows, :] = term + up(recv_a[s, m, x, rows, :])

        def stage_c(u):
            s = odd(u)
            free(send_c.at[s], sc.at[s], u >= 2)
            for m in THREE:
                copy_b(u, m).wait_recv()
                send_c[s, m] = (own_b[s, m] + up(recv_b[lax.rem(u, 4), m])).astype(BF)
                copy_c(u, m).start()

        def stage_d(u):
            s = odd(u)
            free(recv_b.at[0], outs_sem.at[s], u >= 2)
            for m in THREE:
                copy_c(u, m).wait_recv()
                total = (up(send_c[s, m]) + up(recv_c[lax.rem(u, 4), m])).astype(BF)
                if m < 2:
                    out_gu[s, m] = total
                else:
                    for k in PAIR:
                        out_d[s, :, C * k : C * (k + 1)] = total[STRIP * k : STRIP * (k + 1)]
                sq[m] += jnp.sum((up(total) * up(total)).reshape(C // 8, 8, C), axis=0)
                outs(u, m)

        def travel(u, event, when):
            for stage, lag in (((stage_c, 3),), ((stage_a, 1), (stage_d, 4)), ((stage_b, 1),))[event]:
                @pl.when(when & (u >= lag))
                def _():
                    stage(u - lag)

        def load0(p, slot):
            return move(wd0_hbm.at[p], wd.at[slot], wsem.at[slot, 2])

        def saved(p, t):
            return [move(src.at[p, ds(t * LONG, LONG)], da.at[ds(t * LONG, LONG), pl.ds(C * i, C)], tsem.at[t, i]) for i, src in enumerate((gate_hbm, up_hbm))]

        def dyin(t):
            return move(dy_hbm.at[ds(t * T, T)], dy.at[ds(t * T, T)], isem.at[0, t])

        def new(t):
            return move(a0_hbm.at[t], a.at[t], isem.at[1, t])

        def arithmetic(rows, dt, act, dg, du):
            def pointwise(block, i, gate_and_up):
                for k in range(0, R, PB):
                    (g, u), d, there = gate_and_up(k), up(dt[odd_of(block, i), k : k + PB].astype(BF)), slice(R * i + k, R * i + k + PB)
                    sig = 1.0 / (1.0 + jnp.exp(-g))
                    silu = g * sig
                    act[block][there] = (silu * u).astype(BF)
                    du[block][there] = (d * silu).astype(BF)
                    dg[block][there] = (d * u * (sig + silu * (1.0 - sig))).astype(BF)

            def odd_of(block, i):
                return i if rows == T else block

            def weight_grads(block, k, u, turned=False, row=None):
                s, n = odd(u + 2), k if row is None else row
                dyt = dy[ds(n * rows, rows), :]
                at, how = (a[n], NN) if turned else (a[n // 2, R * block : R * (block + 1), :], TN)
                acc_g[s] = jnp.where(k == 0, 0.0, acc_g[s]) + dot(at, dg[block][...], how)
                acc_u[s] = jnp.where(k == 0, 0.0, acc_u[s]) + dot(at, du[block][...], how)
                acc_d[s] = jnp.where(k == 0, 0.0, acc_d[s]) + dot(act[block][...], dyt, TN)

            return pointwise, weight_grads

        def last_layer(wgu, gt, ut, dt, act0, act1, dg0, dg1, du0, du1):
            dg, du = (dg0, dg1), (du0, du1)
            pointwise, weight_grads = arithmetic(R, dt, (act0, act1), dg, du)

            def loads(p, slot, wait):
                for ref, sem in ((wgu.at[slot], wsem.at[slot, 0]), (wd.at[slot], wsem.at[slot, 1])):
                    if wait:
                        move(ref, ref, sem).wait()
                if wait:
                    return

                def go(src, dst, k):
                    move(src, dst, wsem.at[slot, k]).start()

                for m in PAIR:
                    for k in PAIR:
                        go(shards[m].at[1, :, ds((p + NC * k) * STRIP, STRIP)], wgu.at[slot, m, ds(C * me, C), pl.ds(STRIP * k, STRIP)], 0)
                for owner in (g1.sib, g1.xn, g1.diagonal):
                    go(g1.block(p, owner, g1.whole), wgu.at[slot, :, ds(C * owner, C), :], 0)
                for i in PAIR:
                    there = wd.at[slot, ds(STRIP * x + PART * i, PART), :]
                    g1.mine(p, i, lambda: go(g1.shard_rows(p, i), there, 1), lambda: go(g1.rows(p, i, x), there, 1))
                go(wd1_hbm.at[p, ds(STRIP * (1 - x), STRIP), :], wd.at[slot, ds(STRIP * (1 - x), STRIP), :], 1)

            neighbours = ("sib", "xn", "yn")
            for which in neighbours:
                pl.semaphore_signal(inside, inc=1, device_id=peers[which], device_id_type=MESH)
            g1.arrived(0)
            loads(0, 0, False)
            for t in range(TRIPS):
                dyin(t).start()
            sq[...] = jnp.zeros_like(sq)

            def output(j):
                tile(x_hbm, j).wait()
                k, t, h = lax.rem(j, 4), j // 2, odd(j)

                def sums(rows):
                    value = (up(ht[k, rows, :]) + up(da[ds(j * R + rows.start, ROWS), :].astype(BF))).astype(BF)
                    ht[k, rows, :] = value
                    return scale_of(up(value))

                def put(rows, scale):
                    a[t, ds(h * R + rows.start, ROWS), :] = (up(ht[k, rows, :]) * scale).astype(BF)

                passes(R, sums, put, 8)
                tile(h_hbm, j, True).start()

            def norm_back(j):
                tile(h_hbm, j).wait()
                k = lax.rem(j, 4)

                def parts(part):
                    rows = ds(j * R + part.start, ROWS)
                    return rows, up(ht[k, part, :]), up(da[rows, :].astype(BF))

                def sums(part):
                    _, wide, g = parts(part)
                    scale = scale_of(wide)
                    return scale, jnp.sum(g * wide, -1, keepdims=True) * (scale * scale * scale * (1.0 / D))

                def put(part, value):
                    rows, wide, g = parts(part)
                    scale, inner = value
                    dy[rows, :] = (up(dy[rows, :]) + up((g * scale - wide * inner).astype(BF))).astype(BF)

                passes(R, sums, put, 8)

                @pl.when(odd(j) == 1)
                def _():
                    new(j // 2).start()

                @pl.when(j + 4 < TILES)
                def _():
                    tile(h_hbm, j + 4).start()

            def input_grads(i, j, u, row=None):
                w, rows = odd(u + 2), ds((j if row is None else row) * R, R)
                da[rows, :] = jnp.where(u == 0, 0.0, da[rows, :]) + dot(dg[i][...], wgu[w, 0], NT) + dot(du[i][...], wgu[w, 1], NT)

            def chunk1(u):
                w = odd(u)
                loads(u, w, True)

                @pl.when(u == NC - 1)
                def _():
                    for j in range(4):
                        tile(h_hbm, j).start()

                def trip(t):
                    now = 2 * u + t
                    first, last = u == 0, u == NC - 1
                    travel(u, 0, t == 0)
                    travel(u, 1, t == 1)

                    @pl.when(first)
                    def _():
                        for i in range(WIDE):
                            output(WIDE * t + i)
                        for i in PAIR:
                            dyin(2 * t + i).wait()

                    @pl.when(now == 2)
                    def _():
                        pl.semaphore_wait(inside, len(neighbours))
                        for j in range(TILES - WIDE, TILES):
                            tile(h_hbm, j, True).wait()

                    @pl.when(EARLY + now < NC)
                    def _():
                        g1.pass_on(EARLY + now)

                    @pl.when((t == 1) & (u + 1 < NC))
                    def _():
                        g1.arrived(u + 1)
                        loads(u + 1, 1 - w, False)

                    @pl.when((t == 1) & last)
                    def _():
                        load0(0, 1 - w).start()
                        for j in range(WIDE - 1):
                            norm_back(j)

                    for i in range(WIDE):
                        j, b, part = WIDE * t + i, i % 2, slice(i % 2 * R, (i % 2 + 1) * R)
                        at, dyt = a[2 * t + i // 2, part, :], dy[ds(j * R, R), :]
                        gt[b] = dot(at, wgu[w, 0], NN)
                        ut[b] = dot(at, wgu[w, 1], NN)
                        dt[b] = dot(dyt, wd[w], NT)
                        pj, pu = before(j, u, TILES)
                        row = jnp.where((now == 0) & (i == 0), 1 - b, pj)
                        input_grads(1 - b, pj, pu, row)
                        weight_grads(1 - b, pj, pu, False, row)
                        pointwise(b, 0, lambda k: (gt[b, k : k + PB], ut[b, k : k + PB]))

                    @pl.when(now == 0)
                    def _():
                        for j in range(WIDE):
                            tile(h_hbm, j, True).wait()
                            tile(x_hbm, j + WIDE).start()

                    travel(u, 2, t == 1)

                loop(0, N // LONG, trip)

            loop(0, NC, chunk1)
            input_grads(1, TILES - 1, NC - 1)
            weight_grads(1, TILES - 1, NC - 1)
            norm_back(WIDE - 1)
            for copy in saved(0, 0):
                copy.start()
            for j in range(WIDE, TILES):
                norm_back(j)

        def first_backward(dt, act0, act1, dg0, dg1, du0, du1):
            pointwise, weight_grads = arithmetic(T, dt, (act0, act1), (dg0, dg1), (du0, du1))
            for ref in (act1, dg1, du1):
                ref[...] = jnp.zeros_like(ref)

            def chunk0(u):
                w, p = odd(u), u - NC
                load0(p, w).wait()

                @pl.when(p + 1 < NC)
                def _():
                    load0(p + 1, 1 - w).start()

                def trip(t):
                    travel(u, 0, t == 0)
                    travel(u, 1, t == 1)

                    @pl.when(p == 0)
                    def _():
                        for i in PAIR:
                            new(2 * t + i).wait()

                    for copy in saved(p, t):
                        copy.wait()

                    @pl.when((t == 0) | (p + 1 < NC))
                    def _():
                        for copy in saved(p + t, 1 - t):
                            copy.start()

                    for block in PAIR:
                        k = 2 * t + block
                        for i in PAIR:
                            dt[i] = dot(dy[ds(k * T + i * R, R), :], wd[w], NT)
                            if i == 0:
                                pk, pu = before(k, u, TRIPS)
                                weight_grads(1 - block, pk, pu, True, jnp.where((p == 0) & (k == 0), 0, pk))

                            def gate_and_up(part):
                                rows = ds(k * T + i * R + part, PB)
                                return da[rows, :C], da[rows, C : 2 * C]

                            pointwise(block, i, gate_and_up)

                    travel(u, 2, t == 1)

                loop(0, N // LONG, trip)

            loop(NC, 2 * NC, chunk0)
            weight_grads(1, TRIPS - 1, 2 * NC - 1, True)

        f, third = pltpu.VMEM, pltpu.VMEM((2, R, C), F32)
        pl.run_scoped(last_layer, f((2, 2, D, C), BF), *[third] * 3, *[f((R, C), BF)] * 6)
        pl.run_scoped(first_backward, third, *[f((T, C), BF)] * 6)

        L = 2 * NC - 1
        for stage, u in ((stage_a, L), (stage_c, L - 2), (stage_d, L - 3), (stage_b, L), (stage_c, L - 1), (stage_d, L - 2), (stage_c, L), (stage_d, L - 1), (stage_d, L)):
            stage(u)
        free(send_a, sa)
        for s in PAIR:
            free(send_b.at[s], sb.at[s])
            free(send_c.at[s], sc.at[s])
        squares = sq[0] + sq[1] + sq[2]
        sqs[me] = squares[:, :STRIP] + squares[:, STRIP:]
        others = [pltpu.make_async_remote_copy(sqs.at[me], sqs.at[me], fsem.at[k], dsem.at[2 + k], device_id=peers[which], device_id_type=MESH)
                  for k, which in enumerate(("sib", "xn", "diagonal"))]
        for copy in others:
            copy.start()
        g1.finish()
        for copy in others:
            copy.wait()
        mean = jnp.sum(sqs[...]) / (3.0 * 2 * D * FF)
        factor = jnp.minimum(1.0, 0.5 * lax.rsqrt(jnp.full((8, STRIP), mean) + 1e-30))
        factor_ref[0, 0] = jnp.max(factor)
        for s in PAIR:
            free(recv_b.at[0], outs_sem.at[s])
        for layer in PAIR:
            got = gd_hbm.at[layer, :, ds(HALF * (1 - c), HALF)]
            move(got, got, dsem.at[layer]).wait()

    piece, f = (3, C, C), pltpu.VMEM
    pl.run_scoped(
        rest,
        f((N, D), BF), f((2, C, D), BF), f((2, D, C), F32), f((2, D, C), F32), f((2, C, D), F32),
        f((3, 2, C, C), BF), f((2, 3, 2, C, C), BF), f((2,) + piece, F32),
        f((2,) + piece, BF), f((4,) + piece, BF), f((2,) + piece, BF), f((4,) + piece, BF), f((2, 2, C, C), BF), f((2, STRIP, HALF), BF),
    )


def gradients(x, dy, *shards):
    dma, shape = pltpu.SemaphoreType.DMA, jax.ShapeDtypeStruct
    sides = [[dma((kinds, NC)), dma((kinds, 2 * NC)), dma((10,))] for kinds in (3, 2)]
    return pl.pallas_call(
        kernel,
        name="gradients",
        in_specs=[ANY] * 5,
        out_specs=[ANY] * 10 + [pl.BlockSpec(memory_space=pltpu.SMEM)],
        out_shape=[shape((N, D), BF), shape((TRIPS, D, T), BF), shape((NC, N, C), F32), shape((NC, N, C), F32),
                   shape((NC, C, D), BF), shape((NC, 2, D, C), BF), shape((NC, C, D), BF),
                   shape((2, C, FF), BF), shape((2, C, FF), BF), shape((2, FF // 4, D), BF), shape((1, 1), F32)],
        scratch_shapes=[
            pltpu.VMEM((TRIPS, T, D), BF), pltpu.VMEM((N, D), F32), pltpu.VMEM((4, R, D), BF),
            pltpu.VMEM((3, 8, C), F32), pltpu.VMEM((4, 8, STRIP), F32),
            dma((2, TILES)), *[dma((2, 2))] * 2, dma((2, 3)), dma((2, 4)), dma((NC, 3)), *sides[0], *sides[1], dma((2,)), dma((5,)),
            dma((2, 3)), dma((4, 3)), dma((4, 3)), dma(()), dma((2,)), dma((2,)), dma((4,)), pltpu.SemaphoreType.REGULAR,
        ],
        compiler_params=pltpu.CompilerParams(vmem_limit_bytes=67_000_000, collective_id=0, has_side_effects=True),
    )(x, dy, *shards)[-4:]


def adamw(w, m, v, g):
    m = 0.9 * m + 0.1 * g
    v = 0.95 * v + 0.05 * g * g
    step = m * lax.rsqrt(v + 1e-8) + 0.1 * w
    return (w - 0.02 * step).astype(BF), m, v


def solution(mesh):
    def step(x, dy, *arrays):
        weights, m, v = (arrays[i : i + 3] for i in (0, 3, 6))
        *grads, factor = gradients(x[0], dy[0], *weights)
        new = [adamw(up(w), m, v, up(g) * factor[0, 0]) for w, m, v, g in zip(weights, m, v, grads, strict=True)]
        return tuple(one[which] for which in THREE for one in new)

    states, cut = P(("rep", "r", "s"), None, None), P(None, "s", None)
    return jax.shard_map(
        step,
        mesh=mesh,
        in_specs=(states, states) + (cut,) * 9,
        out_specs=(P("rep", "s", None),) * 9,
        check_vma=False,
    )
```

```python
import functools

import jax
import jax.numpy as jnp
from jax import lax
from jax.experimental import pallas as pl
from jax.experimental.pallas import tpu as pltpu
from jax.sharding import PartitionSpec as P

MESH = pl.DeviceIdType.MESH
BF, F32 = jnp.bfloat16, jnp.float32
ANY = pl.BlockSpec(memory_space=pl.ANY)
NN = (((1,), (0,)), ((), ()))
NT = (((1,), (1,)), ((), ()))
TN = (((0,), (0,)), ((), ()))
PAIR, THREE = range(2), range(3)
N, D, FF = 4096, 1024, 2816
STRIP, PART = 128, 64
C = 2 * STRIP
NC = FF // C
R = 512
T = 2 * R
TRIPS, TILES = N // T, N // R
WIDE = 4
LONG = WIDE * R
HALF = D // 2
ROWS, PB = 16, 32
EPS = 1e-6
EARLY, AT = 4, 13


def dot(a, b, how):
    return lax.dot_general(a, b, how, preferred_element_type=F32)


def ds(start, size):
    return pl.ds(pl.multiple_of(start, size), size)


def up(v):
    return v.astype(F32)


def odd(v):
    return lax.rem(v, 2)


def loop(first, last, body):
    def step(i, nothing):
        body(i)
        return nothing

    lax.fori_loop(first, last, step, 0)


def passes(count, prepare, finish, unroll):
    def step(i):
        parts = [ds((i * unroll + k) * ROWS, ROWS) for k in range(unroll)]
        ready = [prepare(rows) for rows in parts]
        for rows, value in zip(parts, ready):
            finish(rows, value)

    loop(0, count // (ROWS * unroll), step)


def before(j, u, count):
    return jnp.where(j == 0, count - 1, j - 1), jnp.where(j == 0, u - 1, u)


def scale_of(wide):
    return lax.rsqrt(jnp.mean(wide * wide, -1, keepdims=True) + EPS)


class Gather:
    def __init__(self, layer, shards, gu, wd, sems, sends, halves):
        self.layer, self.shards, self.gu, self.wd, self.halves = layer, shards, gu, wd, halves
        self.sems, self.sends = sems, sends
        self.me, self.y = lax.axis_index("s"), lax.axis_index("r")
        self.x, self.c = self.me // 2, odd(self.me)
        self.sib, self.xn = self.me + 1 - 2 * self.c, lax.rem(self.me + 2, 4)
        self.diagonal = self.xn + 1 - 2 * self.c
        self.peers = {"sib": {"s": self.sib}, "xn": {"s": self.xn}, "yn": {"r": 1 - self.y}, "diagonal": {"s": self.diagonal}}
        self.whole = (0, C)

    def far(self, src, dst, kind, where, which):
        row = kind % 5
        sem = self.sems[kind // 5].at[row if row < 3 else 0, where]
        return pltpu.make_async_remote_copy(src, dst, self.sends.at[kind], sem, device_id=self.peers[which], device_id_type=MESH)

    def strips(self, p, part):
        start, size = part
        for m in PAIR:
            for k in PAIR:
                yield (self.shards[m].at[self.layer, ds(start, size), ds((p + NC * k) * STRIP, STRIP)],
                       self.gu.at[p, m, ds(C * self.me + start, size), pl.ds(STRIP * k, STRIP)])

    def block(self, p, owner, part):
        start, size = part
        return self.gu.at[p, :, ds(C * owner + start, size), :]

    def owner(self, p, i):
        return (2 * p + i) // NC

    def shard_rows(self, p, i):
        return self.shards[2].at[self.layer, ds((2 * p + i - NC * self.c) * PART, PART), :]

    def rows(self, p, i, x, half=None):
        rows = ds(STRIP * x + PART * i, PART)
        return self.wd.at[p, rows, :] if half is None else self.wd.at[p, rows, ds(HALF * half, HALF)]

    def mine(self, p, i, yes, no=None):
        pl.when(self.owner(p, i) == self.c)(yes)
        if no is not None:
            pl.when(self.owner(p, i) != self.c)(no)

    def part(self, h):
        return (STRIP * h, STRIP) if self.halves else self.whole

    def half(self, h):
        return h if self.halves else None

    def issue(self, p):
        for src, dst in self.strips(p, self.part(self.y)):
            self.far(src, dst, 1, p, "xn").start()
        for i in PAIR:
            def send(i=i):
                src = self.shard_rows(p, i)
                if self.halves:
                    src = src.at[:, ds(HALF * self.y, HALF)]
                self.far(src, self.rows(p, i, self.x, self.half(self.y)), 6, 2 * p + i, "xn").start()
            self.mine(p, i, send)

    def issue_near(self, p):
        for src, dst in self.strips(p, self.whole):
            self.far(src, dst, 0, p, "sib").start()
        for i in PAIR:
            def send(i=i):
                self.far(self.shard_rows(p, i), self.rows(p, i, self.x), 5, 2 * p + i, "sib").start()
            self.mine(p, i, send)

    def pass_on(self, p):
        block = self.block(p, self.xn, self.part(self.y))
        self.far(block, block, 1, p, "xn").wait_recv()
        if self.halves:
            self.far(block, block, 2, p, "yn").start()
        self.far(block, block, 3, p, "sib").start()
        for i in PAIR:
            def send(i=i):
                rows = self.rows(p, i, 1 - self.x, self.half(self.y))
                self.far(rows, rows, 6, 2 * p + i, "xn").wait_recv()
                if self.halves:
                    self.far(rows, rows, 7, 2 * p + i, "yn").start()
                self.far(rows, rows, 8, 2 * p + i, "sib").start()
            self.mine(p, i, send)

    def pass_on_y(self, p):
        block = self.block(p, self.xn, self.part(1 - self.y))
        self.far(block, block, 2, p, "yn").wait_recv()
        self.far(block, block, 4, p, "sib").start()
        for i in PAIR:
            def send(i=i):
                rows = self.rows(p, i, 1 - self.x, 1 - self.y)
                self.far(rows, rows, 7, 2 * p + i, "yn").wait_recv()
                self.far(rows, rows, 9, 2 * p + i, "sib").start()
            self.mine(p, i, send)

    def arrived(self, p):
        block = self.gu.at[p, :, pl.ds(0, 2 * C), :]
        self.far(block, block, 0, p, "sib").wait_recv()
        for i in PAIR:
            def wait(i=i):
                rows = self.wd.at[p, pl.ds(0, STRIP), :]
                self.far(rows, rows, 5, 2 * p + i, "sib").wait_recv()
            pl.when(self.owner(p, i) != self.c)(wait)

    def finish(self):
        for kind in (range(10) if self.halves else (0, 1, 3, 5, 6, 8)):
            all_rows = kind in (0, 5) or not self.halves
            if kind < 5:
                block = self.gu.at[:, :, pl.ds(0, C if all_rows else STRIP), :]
            else:
                block = self.wd.at[:, pl.ds(0, PART), :] if all_rows else self.wd.at[:, pl.ds(0, PART), pl.ds(0, HALF)]
            self.far(block, block, kind, 0, "sib").wait_send()


def kernel(x_hbm, dy_hbm, w_gate, w_up, w_down,
           h_hbm, a0_hbm, gate_hbm, up_hbm, wd0_hbm, gu1_hbm, wd1_hbm, gg_hbm, gu_hbm, gd_hbm, factor_ref,
           a, da, ht, sq, sqs,
           isem, osem, tsem, wsem, xsem, own, gsem0, dsem0, sends0, gsem1, dsem1, sends1, outs_sem, dsem, ra, rb, rc, sa, sb, sc, fsem, inside):
    shards = (w_gate, w_up, w_down)
    g1 = Gather(1, shards, gu1_hbm, wd1_hbm, (gsem1, dsem1), sends1, False)
    me, x, c, peers = g1.me, g1.x, g1.c, g1.peers

    def move(src, dst, sem):
        return pltpu.make_async_copy(src, dst, sem)

    def tile(hbm, j, back=False):
        k = lax.rem(j, 4)
        there, here = hbm.at[ds(j * R, R)], ht.at[k]
        return move(here, there, xsem.at[1, k]) if back else move(there, here, xsem.at[0, k])

    def first_layer(gu, wd, xt, gt, ut, *act):
        g0 = Gather(0, shards, gu, wd, (gsem0, dsem0), sends0, True)

        def saves(p, t, slot):
            return [move(src.at[slot], dst.at[p, ds(t * LONG, LONG)], osem.at[slot, i]) for i, (src, dst) in enumerate(((gt, gate_hbm), (ut, up_hbm)))]

        def local(p, wait):
            if wait:
                block = g0.block(p, me, g0.whole)
                move(block, block, own.at[p, 2]).wait()
            else:
                for src, dst in g0.strips(p, g0.whole):
                    move(src, dst, own.at[p, 2]).start()
            for i in PAIR:
                def go(i=i):
                    copy = move(g0.shard_rows(p, i), g0.rows(p, i, x), own.at[p, i])
                    copy.wait() if wait else copy.start()
                g0.mine(p, i, go)

        def keep(p):
            return move(wd.at[p], wd0_hbm.at[p], fsem.at[3])

        xin = [move(x_hbm.at[pl.ds(t * T, T)], a.at[t], isem.at[0, t]) for t in range(TRIPS)]
        turned = [move(xt.at[odd_], a0_hbm.at[t, :, pl.ds(R * odd_, R)], isem.at[1, 2 * t + odd_]) for t in range(TRIPS) for odd_ in PAIR]
        for copy in xin:
            copy.start()
        barrier = pltpu.get_barrier_semaphore()
        for peer in peers.values():
            pl.semaphore_signal(barrier, inc=1, device_id=peer, device_id_type=MESH)
        pl.semaphore_wait(barrier, len(peers))

        def issue0(p):
            g0.issue(p)

            @pl.when(p < 2)
            def _():
                g0.issue_near(p)
                local(p, False)

        loop(0, 2, issue0)
        for t in range(TRIPS):
            xin[t].wait()

            def put(rows, scale):
                a[t, rows, :] = (up(a[t, rows, :]) * scale).astype(BF)

            passes(T, lambda rows: scale_of(up(a[t, rows, :])), put, 8)
            for h in PAIR:
                if t >= 1:
                    turned[2 * t + h - 2].wait()
                for k in PAIR:
                    xt[h, :, C * k : C * (k + 1)] = a[t, R * h + C * k : R * h + C * (k + 1), :].T
                turned[2 * t + h].start()
            if t == 0:
                loop(2, NC, issue0)
            if t == 1:
                g0.pass_on(0)
            if t == 2:
                g0.pass_on(1)
        g0.pass_on_y(0)

        def down(i, j, p):
            rows = ds(j * R, R)
            da[rows, :] = jnp.where(p == 0, 0.0, da[rows, :]) + dot(act[i][...], wd[jnp.maximum(p, 0)], NN)

        def chunk(p):
            def trip(t):
                now = 2 * p + t

                @pl.when((now >= 1) & (now + 1 < NC))
                def _():
                    g0.pass_on(now + 1)

                @pl.when((now == 1) | (now >= 3) & (now <= NC))
                def _():
                    g0.pass_on_y(jnp.maximum(now - 1, 1))

                @pl.when(now + 2 < NC)
                def _():
                    g0.issue_near(now + 2)
                    local(now + 2, False)

                @pl.when(now < NC)
                def _():
                    g1.issue(now)

                @pl.when(now >= NC)
                def _():
                    g1.issue_near(now - NC)

                @pl.when(now == 2 * NC - 1)
                def _():
                    for j in range(WIDE):
                        tile(x_hbm, j).start()

                early = (2 * (now - AT) + 4) // 5

                @pl.when((now >= AT) & ((5 * early) // 2 == now - AT) & (early < EARLY))
                def _():
                    g1.pass_on(early)

                @pl.when(t == 0)
                def _():
                    local(p, True)
                    g0.arrived(p)
                    keep(p).start()

                @pl.when(now >= 2)
                def _():
                    for copy in saves(0, 0, t):
                        copy.wait()

                for i in range(WIDE):
                    part, j = pl.ds(i * R, R), WIDE * t + i
                    at = a[2 * t + i // 2, i % 2 * R : (i % 2 + 1) * R, :]
                    gt[t, part] = dot(at, gu[p, 0], NN)
                    ut[t, part] = dot(at, gu[p, 1], NN)
                    down(1 - i % 2, *before(j, p, TILES))
                    for k in range(0, R, PB):
                        g, u = gt[t, pl.ds(i * R + k, PB)], ut[t, pl.ds(i * R + k, PB)]
                        act[i % 2][k : k + PB] = (g / (1.0 + jnp.exp(-g)) * u).astype(BF)
                for copy in saves(p, t, t):
                    copy.start()

            loop(0, N // LONG, trip)

        loop(0, NC, chunk)
        down(1, TILES - 1, NC - 1)
        for copy in turned[-2:]:
            copy.wait()
        for o in PAIR:
            for copy in saves(0, 0, o):
                copy.wait()
        move(wd, wd0_hbm, fsem.at[3]).wait()
        g0.finish()

    pl.run_scoped(first_layer, pltpu.VMEM((NC, 2, D, C), BF), pltpu.VMEM((NC, C, D), BF), pltpu.VMEM((2, D, R), BF), *[pltpu.VMEM((2, LONG, C), F32)] * 2, *[pltpu.VMEM((R, C), BF)] * 2)

    def rest(dy, wd, acc_g, acc_u, acc_d, send_a, recv_a, own_b, send_b, recv_b, send_c, recv_c, out_gu, out_d):
        L = 2 * NC - 1

        def copy_a(u, m):
            return pltpu.make_async_remote_copy(send_a.at[m], recv_a.at[odd(u), m], sa, ra.at[odd(u), m], device_id=peers["sib"], device_id_type=MESH)

        def copy_b(u, m):
            s, q = odd(u), lax.rem(u, 4)
            return pltpu.make_async_remote_copy(send_b.at[s, m], recv_b.at[q, m], sb.at[s], rb.at[q, m], device_id=peers["xn"], device_id_type=MESH)

        def copy_c(u, m):
            s, q = odd(u), lax.rem(u, 4)
            return pltpu.make_async_remote_copy(send_c.at[s, m], recv_c.at[q, m], sc.at[s], rc.at[q, m], device_id=peers["yn"], device_id_type=MESH)

        def free(ref, sem, when=True):
            pl.when(when)(lambda: move(ref, ref, sem).wait())

        def outs(u, m):
            s, layer, p = odd(u), 1 - u // NC, lax.rem(u, NC)
            sem = outs_sem.at[s]
            for i in PAIR:
                if m < 2:
                    move(out_gu.at[s, m, :, pl.ds(STRIP * i, STRIP)], (gg_hbm, gu_hbm)[m].at[layer, :, ds((p + NC * i) * STRIP, STRIP)], sem).start()
                    continue
                src = out_d.at[s, pl.ds(PART * i, PART), :]
                dst = gd_hbm.at[layer, ds((2 * p + i - NC * g1.owner(p, i)) * PART, PART), ds(HALF * c, HALF)]
                g1.mine(p, i, lambda: move(src, dst, sem).start(),
                        lambda: pltpu.make_async_remote_copy(src, dst, sem, dsem.at[layer], device_id=peers["sib"], device_id_type=MESH).start())

        def part(s, m, xd, cc):
            if m < 2:
                return [(pl.ds(0, C), (acc_g, acc_u)[m][s, ds(2 * C * xd + C * cc, C), :])]
            return [(pl.ds(STRIP * k, STRIP), acc_d[s, ds(STRIP * xd, STRIP), ds(HALF * cc + C * k, C)]) for k in PAIR]

        def stage_a(u):
            free(send_a, sa, u >= 1)
            for m in THREE:
                for xd in PAIR:
                    for rows, term in part(odd(u), m, xd, 1 - c):
                        send_a[m, xd, rows, :] = term.astype(BF)
                copy_a(u, m).start()

        def stage_b(u):
            s = odd(u)
            free(send_b.at[s], sb.at[s], u >= 2)
            for m in THREE:
                copy_a(u, m).wait_recv()
                for rows, term in part(s, m, 1 - x, c):
                    send_b[s, m, rows, :] = (term + up(recv_a[s, m, 1 - x, rows, :])).astype(BF)
                copy_b(u, m).start()
            for m in THREE:
                for rows, term in part(s, m, x, c):
                    own_b[s, m, rows, :] = term + up(recv_a[s, m, x, rows, :])

        def stage_c(u):
            s = odd(u)
            free(send_c.at[s], sc.at[s], u >= 2)
            for m in THREE:
                copy_b(u, m).wait_recv()
                send_c[s, m] = (own_b[s, m] + up(recv_b[lax.rem(u, 4), m])).astype(BF)
                copy_c(u, m).start()

        def stage_d(u):
            s = odd(u)
            free(recv_b.at[0], outs_sem.at[s], u >= 2)
            for m in THREE:
                copy_c(u, m).wait_recv()
                total = (up(send_c[s, m]) + up(recv_c[lax.rem(u, 4), m])).astype(BF)
                if m < 2:
                    out_gu[s, m] = total
                else:
                    for k in PAIR:
                        out_d[s, :, C * k : C * (k + 1)] = total[STRIP * k : STRIP * (k + 1)]
                sq[m] += jnp.sum((up(total) * up(total)).reshape(C // 8, 8, C), axis=0)
                outs(u, m)

        def travel(u, event, when):
            for stage, lag in (((stage_c, 3),), ((stage_a, 1), (stage_d, 4)), ((stage_b, 1),))[event]:
                @pl.when(when & (u >= lag))
                def _():
                    stage(u - lag)

        def load0(p, slot):
            return move(wd0_hbm.at[p], wd.at[slot], wsem.at[slot, 2])

        def saved(p, t):
            return [move(src.at[p, ds(t * LONG, LONG)], da.at[ds(t * LONG, LONG), pl.ds(C * i, C)], tsem.at[t, i]) for i, src in enumerate((gate_hbm, up_hbm))]

        def dyin(t):
            return move(dy_hbm.at[ds(t * T, T)], dy.at[ds(t * T, T)], isem.at[0, t])

        def new(t):
            return move(a0_hbm.at[t], a.at[t], isem.at[1, t])

        def arithmetic(rows, dt, act, dg, du):
            def pointwise(block, i, gate_and_up):
                for k in range(0, R, PB):
                    (g, u), d, there = gate_and_up(k), up(dt[odd_of(block, i), k : k + PB].astype(BF)), slice(R * i + k, R * i + k + PB)
                    sig = 1.0 / (1.0 + jnp.exp(-g))
                    silu = g * sig
                    act[block][there] = (silu * u).astype(BF)
                    du[block][there] = (d * silu).astype(BF)
                    dg[block][there] = (d * u * (sig + silu * (1.0 - sig))).astype(BF)

            def odd_of(block, i):
                return i if rows == T else block

            def weight_grads(block, k, u, turned=False, row=None):
                s, n = odd(u + 2), k if row is None else row
                dyt = dy[ds(n * rows, rows), :]
                at, how = (a[n], NN) if turned else (a[n // 2, R * block : R * (block + 1), :], TN)
                acc_g[s] = jnp.where(k == 0, 0.0, acc_g[s]) + dot(at, dg[block][...], how)
                acc_u[s] = jnp.where(k == 0, 0.0, acc_u[s]) + dot(at, du[block][...], how)
                acc_d[s] = jnp.where(k == 0, 0.0, acc_d[s]) + dot(act[block][...], dyt, TN)

            return pointwise, weight_grads

        def last_layer(wgu, gt, ut, dt, act0, act1, dg0, dg1, du0, du1):
            dg, du = (dg0, dg1), (du0, du1)
            pointwise, weight_grads = arithmetic(R, dt, (act0, act1), dg, du)

            def loads(p, slot, wait):
                for ref, sem in ((wgu.at[slot], wsem.at[slot, 0]), (wd.at[slot], wsem.at[slot, 1])):
                    if wait:
                        move(ref, ref, sem).wait()
                if wait:
                    return

                def go(src, dst, k):
                    move(src, dst, wsem.at[slot, k]).start()

                for m in PAIR:
                    for k in PAIR:
                        go(shards[m].at[1, :, ds((p + NC * k) * STRIP, STRIP)], wgu.at[slot, m, ds(C * me, C), pl.ds(STRIP * k, STRIP)], 0)
                for owner in (g1.sib, g1.xn, g1.diagonal):
                    go(g1.block(p, owner, g1.whole), wgu.at[slot, :, ds(C * owner, C), :], 0)
                for i in PAIR:
                    there = wd.at[slot, ds(STRIP * x + PART * i, PART), :]
                    g1.mine(p, i, lambda: go(g1.shard_rows(p, i), there, 1), lambda: go(g1.rows(p, i, x), there, 1))
                go(wd1_hbm.at[p, ds(STRIP * (1 - x), STRIP), :], wd.at[slot, ds(STRIP * (1 - x), STRIP), :], 1)

            neighbours = ("sib", "xn", "yn")
            for which in neighbours:
                pl.semaphore_signal(inside, inc=1, device_id=peers[which], device_id_type=MESH)
            g1.arrived(0)
            loads(0, 0, False)
            for t in range(TRIPS):
                dyin(t).start()
            sq[...] = jnp.zeros_like(sq)

            def output(j):
                tile(x_hbm, j).wait()
                k, t, h = lax.rem(j, 4), j // 2, odd(j)

                def sums(rows):
                    value = (up(ht[k, rows, :]) + up(da[ds(j * R + rows.start, ROWS), :].astype(BF))).astype(BF)
                    ht[k, rows, :] = value
                    return scale_of(up(value))

                def put(rows, scale):
                    a[t, ds(h * R + rows.start, ROWS), :] = (up(ht[k, rows, :]) * scale).astype(BF)

                passes(R, sums, put, 16)
                tile(h_hbm, j, True).start()

            def norm_back(j):
                tile(h_hbm, j).wait()
                k = lax.rem(j, 4)

                def parts(part):
                    rows = ds(j * R + part.start, ROWS)
                    return rows, up(ht[k, part, :]), up(da[rows, :].astype(BF))

                def sums(part):
                    _, wide, g = parts(part)
                    scale = scale_of(wide)
                    return scale, jnp.sum(g * wide, -1, keepdims=True) * (scale * scale * scale * (1.0 / D))

                def put(part, value):
                    rows, wide, g = parts(part)
                    scale, inner = value
                    dy[rows, :] = (up(dy[rows, :]) + up((g * scale - wide * inner).astype(BF))).astype(BF)

                passes(R, sums, put, 8)

                @pl.when(odd(j) == 1)
                def _():
                    new(j // 2).start()

                @pl.when(j + 4 < TILES)
                def _():
                    tile(h_hbm, j + 4).start()

            def input_grads(i, j, u, row=None):
                w, rows = odd(u + 2), ds((j if row is None else row) * R, R)
                da[rows, :] = jnp.where(u == 0, 0.0, da[rows, :]) + dot(dg[i][...], wgu[w, 0], NT) + dot(du[i][...], wgu[w, 1], NT)

            def chunk1(u):
                w = odd(u)
                loads(u, w, True)

                @pl.when(u == NC - 1)
                def _():
                    for j in range(4):
                        tile(h_hbm, j).start()

                def trip(t):
                    now = 2 * u + t
                    first, last = u == 0, u == NC - 1
                    travel(u, 0, t == 0)
                    travel(u, 1, t == 1)

                    @pl.when(first)
                    def _():
                        for i in range(WIDE):
                            output(WIDE * t + i)
                        for i in PAIR:
                            dyin(2 * t + i).wait()

                    @pl.when(now == 2)
                    def _():
                        pl.semaphore_wait(inside, len(neighbours))
                        for j in range(TILES - WIDE, TILES):
                            tile(h_hbm, j, True).wait()

                    @pl.when(EARLY + now < NC)
                    def _():
                        g1.pass_on(EARLY + now)

                    @pl.when((t == 1) & (u + 1 < NC))
                    def _():
                        g1.arrived(u + 1)
                        loads(u + 1, 1 - w, False)

                    @pl.when((t == 1) & last)
                    def _():
                        load0(0, 1 - w).start()
                        for j in range(WIDE - 1):
                            norm_back(j)

                    for i in range(WIDE):
                        j, b, part = WIDE * t + i, i % 2, slice(i % 2 * R, (i % 2 + 1) * R)
                        at, dyt = a[2 * t + i // 2, part, :], dy[ds(j * R, R), :]
                        gt[b] = dot(at, wgu[w, 0], NN)
                        ut[b] = dot(at, wgu[w, 1], NN)
                        dt[b] = dot(dyt, wd[w], NT)
                        pj, pu = before(j, u, TILES)
                        row = jnp.where((now == 0) & (i == 0), 1 - b, pj)
                        input_grads(1 - b, pj, pu, row)
                        weight_grads(1 - b, pj, pu, False, row)
                        pointwise(b, 0, lambda k: (gt[b, k : k + PB], ut[b, k : k + PB]))

                    @pl.when(now == 0)
                    def _():
                        for j in range(WIDE):
                            tile(h_hbm, j, True).wait()
                            tile(x_hbm, j + WIDE).start()

                    travel(u, 2, t == 1)

                loop(0, N // LONG, trip)

            loop(0, NC, chunk1)
            input_grads(1, TILES - 1, NC - 1)
            weight_grads(1, TILES - 1, NC - 1)
            norm_back(WIDE - 1)
            for copy in saved(0, 0):
                copy.start()
            for j in range(WIDE, TILES):
                norm_back(j)

        def first_backward(dt, act0, act1, dg0, dg1, du0, du1):
            pointwise, weight_grads = arithmetic(T, dt, (act0, act1), (dg0, dg1), (du0, du1))
            for ref in (act1, dg1, du1):
                ref[...] = jnp.zeros_like(ref)

            def chunk0(u):
                w, p = odd(u), u - NC
                load0(p, w).wait()

                @pl.when(p + 1 < NC)
                def _():
                    load0(p + 1, 1 - w).start()

                def trip(t):
                    travel(u, 0, t == 0)
                    travel(u, 1, t == 1)

                    @pl.when(p == 0)
                    def _():
                        for i in PAIR:
                            new(2 * t + i).wait()

                    for copy in saved(p, t):
                        copy.wait()

                    @pl.when((t == 0) | (p + 1 < NC))
                    def _():
                        for copy in saved(p + t, 1 - t):
                            copy.start()

                    for block in PAIR:
                        k = 2 * t + block
                        for i in PAIR:
                            dt[i] = dot(dy[ds(k * T + i * R, R), :], wd[w], NT)
                            if i == 0:
                                pk, pu = before(k, u, TRIPS)
                                weight_grads(1 - block, pk, pu, True, jnp.where((p == 0) & (k == 0), 0, pk))

                            def gate_and_up(part):
                                rows = ds(k * T + i * R + part, PB)
                                return da[rows, :C], da[rows, C : 2 * C]

                            pointwise(block, i, gate_and_up)

                    travel(u, 2, t == 1)

                loop(0, N // LONG, trip)

            loop(NC, 2 * NC, chunk0)
            stage_c(L - 2)
            weight_grads(1, TRIPS - 1, L, True)

        f, third = pltpu.VMEM, pltpu.VMEM((2, R, C), F32)
        pl.run_scoped(last_layer, f((2, 2, D, C), BF), *[third] * 3, *[f((R, C), BF)] * 6)
        pl.run_scoped(first_backward, third, *[f((T, C), BF)] * 6)

        for stage, u in ((stage_a, L), (stage_d, L - 3), (stage_b, L), (stage_c, L - 1), (stage_d, L - 2), (stage_c, L), (stage_d, L - 1), (stage_d, L)):
            stage(u)
        free(send_a, sa)
        for s in PAIR:
            free(send_b.at[s], sb.at[s])
            free(send_c.at[s], sc.at[s])
        squares = sq[0] + sq[1] + sq[2]
        sqs[me] = squares[:, :STRIP] + squares[:, STRIP:]
        others = [pltpu.make_async_remote_copy(sqs.at[me], sqs.at[me], fsem.at[k], dsem.at[2 + k], device_id=peers[which], device_id_type=MESH)
                  for k, which in enumerate(("sib", "xn", "diagonal"))]
        for copy in others:
            copy.start()
        g1.finish()
        for copy in others:
            copy.wait()
        mean = jnp.sum(sqs[...]) / (3.0 * 2 * D * FF)
        factor = jnp.minimum(1.0, 0.5 * lax.rsqrt(jnp.full((8, STRIP), mean) + 1e-30))
        factor_ref[0, 0] = jnp.max(factor)
        for s in PAIR:
            free(recv_b.at[0], outs_sem.at[s])
        for layer in PAIR:
            got = gd_hbm.at[layer, :, ds(HALF * (1 - c), HALF)]
            move(got, got, dsem.at[layer]).wait()

    piece, f = (3, C, C), pltpu.VMEM
    pl.run_scoped(
        rest,
        f((N, D), BF), f((2, C, D), BF), f((2, D, C), F32), f((2, D, C), F32), f((2, C, D), F32),
        f((3, 2, C, C), BF), f((2, 3, 2, C, C), BF), f((2,) + piece, F32),
        f((2,) + piece, BF), f((4,) + piece, BF), f((2,) + piece, BF), f((4,) + piece, BF), f((2, 2, C, C), BF), f((2, STRIP, HALF), BF),
    )


def gradients(x, dy, *shards):
    dma, shape = pltpu.SemaphoreType.DMA, jax.ShapeDtypeStruct
    sides = [[dma((kinds, NC)), dma((kinds, 2 * NC)), dma((10,))] for kinds in (3, 2)]
    return pl.pallas_call(
        kernel,
        name="gradients",
        in_specs=[ANY] * 5,
        out_specs=[ANY] * 10 + [pl.BlockSpec(memory_space=pltpu.SMEM)],
        out_shape=[shape((N, D), BF), shape((TRIPS, D, T), BF), shape((NC, N, C), F32), shape((NC, N, C), F32),
                   shape((NC, C, D), BF), shape((NC, 2, D, C), BF), shape((NC, C, D), BF),
                   shape((2, C, FF), BF), shape((2, C, FF), BF), shape((2, FF // 4, D), BF), shape((1, 1), F32)],
        scratch_shapes=[
            pltpu.VMEM((TRIPS, T, D), BF), pltpu.VMEM((N, D), F32), pltpu.VMEM((4, R, D), BF),
            pltpu.VMEM((3, 8, C), F32), pltpu.VMEM((4, 8, STRIP), F32),
            dma((2, TILES)), *[dma((2, 2))] * 2, dma((2, 3)), dma((2, 4)), dma((NC, 3)), *sides[0], *sides[1], dma((2,)), dma((5,)),
            dma((2, 3)), dma((4, 3)), dma((4, 3)), dma(()), dma((2,)), dma((2,)), dma((4,)), pltpu.SemaphoreType.REGULAR,
        ],
        compiler_params=pltpu.CompilerParams(vmem_limit_bytes=67_000_000, collective_id=0, has_side_effects=True),
    )(x, dy, *shards)[-4:]


def adamw(w, m, v, g):
    m = 0.9 * m + 0.1 * g
    v = 0.95 * v + 0.05 * g * g
    step = m * lax.rsqrt(v + 1e-8) + 0.1 * w
    return (w - 0.02 * step).astype(BF), m, v


def solution(mesh):
    def step(x, dy, *arrays):
        weights, m, v = (arrays[i : i + 3] for i in (0, 3, 6))
        *grads, factor = gradients(x[0], dy[0], *weights)
        new = [adamw(up(w), m, v, up(g) * factor[0, 0]) for w, m, v, g in zip(weights, m, v, grads, strict=True)]
        return tuple(one[which] for which in THREE for one in new)

    states, cut = P(("rep", "r", "s"), None, None), P(None, "s", None)
    return jax.shard_map(
        step,
        mesh=mesh,
        in_specs=(states, states) + (cut,) * 9,
        out_specs=(P("rep", "s", None),) * 9,
        check_vma=False,
    )
```

```python
import functools

import jax
import jax.numpy as jnp
from jax import lax
from jax.experimental import pallas as pl
from jax.experimental.pallas import tpu as pltpu
from jax.sharding import PartitionSpec as P

MESH = pl.DeviceIdType.MESH
BF, F32 = jnp.bfloat16, jnp.float32
ANY = pl.BlockSpec(memory_space=pl.ANY)
NN = (((1,), (0,)), ((), ()))
NT = (((1,), (1,)), ((), ()))
TN = (((0,), (0,)), ((), ()))
PAIR, THREE = range(2), range(3)
N, D, FF = 4096, 1024, 2816
STRIP, PART = 128, 64
C = 2 * STRIP
NC = FF // C
R = 512
T = 2 * R
TRIPS, TILES = N // T, N // R
WIDE = 4
LONG = WIDE * R
HALF = D // 2
ROWS, PB = 16, 32
EPS = 1e-6
EARLY, AT = 4, 13


def dot(a, b, how):
    return lax.dot_general(a, b, how, preferred_element_type=F32)


def ds(start, size):
    return pl.ds(pl.multiple_of(start, size), size)


def up(v):
    return v.astype(F32)


def odd(v):
    return lax.rem(v, 2)


def loop(first, last, body):
    def step(i, nothing):
        body(i)
        return nothing

    lax.fori_loop(first, last, step, 0)


def passes(count, prepare, finish, unroll):
    def step(i):
        parts = [ds((i * unroll + k) * ROWS, ROWS) for k in range(unroll)]
        ready = [prepare(rows) for rows in parts]
        for rows, value in zip(parts, ready):
            finish(rows, value)

    loop(0, count // (ROWS * unroll), step)


def before(j, u, count):
    return jnp.where(j == 0, count - 1, j - 1), jnp.where(j == 0, u - 1, u)


def scale_of(wide):
    return lax.rsqrt(jnp.mean(wide * wide, -1, keepdims=True) + EPS)


class Gather:
    def __init__(self, layer, shards, gu, wd, sems, sends, halves):
        self.layer, self.shards, self.gu, self.wd, self.halves = layer, shards, gu, wd, halves
        self.sems, self.sends = sems, sends
        self.me, self.y = lax.axis_index("s"), lax.axis_index("r")
        self.x, self.c = self.me // 2, odd(self.me)
        self.sib, self.xn = self.me + 1 - 2 * self.c, lax.rem(self.me + 2, 4)
        self.diagonal = self.xn + 1 - 2 * self.c
        self.peers = {"sib": {"s": self.sib}, "xn": {"s": self.xn}, "yn": {"r": 1 - self.y}, "diagonal": {"s": self.diagonal}}
        self.whole = (0, C)

    def far(self, src, dst, kind, where, which):
        row = kind % 5
        sem = self.sems[kind // 5].at[row if row < 3 else 0, where]
        return pltpu.make_async_remote_copy(src, dst, self.sends.at[kind], sem, device_id=self.peers[which], device_id_type=MESH)

    def strips(self, p, part):
        start, size = part
        for m in PAIR:
            for k in PAIR:
                yield (self.shards[m].at[self.layer, ds(start, size), ds((p + NC * k) * STRIP, STRIP)],
                       self.gu.at[p, m, ds(C * self.me + start, size), pl.ds(STRIP * k, STRIP)])

    def block(self, p, owner, part):
        start, size = part
        return self.gu.at[p, :, ds(C * owner + start, size), :]

    def owner(self, p, i):
        return (2 * p + i) // NC

    def shard_rows(self, p, i):
        return self.shards[2].at[self.layer, ds((2 * p + i - NC * self.c) * PART, PART), :]

    def rows(self, p, i, x, half=None):
        rows = ds(STRIP * x + PART * i, PART)
        return self.wd.at[p, rows, :] if half is None else self.wd.at[p, rows, ds(HALF * half, HALF)]

    def mine(self, p, i, yes, no=None):
        pl.when(self.owner(p, i) == self.c)(yes)
        if no is not None:
            pl.when(self.owner(p, i) != self.c)(no)

    def part(self, h):
        return (STRIP * h, STRIP) if self.halves else self.whole

    def half(self, h):
        return h if self.halves else None

    def issue(self, p):
        for src, dst in self.strips(p, self.part(self.y)):
            self.far(src, dst, 1, p, "xn").start()
        for i in PAIR:
            def send(i=i):
                src = self.shard_rows(p, i)
                if self.halves:
                    src = src.at[:, ds(HALF * self.y, HALF)]
                self.far(src, self.rows(p, i, self.x, self.half(self.y)), 6, 2 * p + i, "xn").start()
            self.mine(p, i, send)

    def issue_near(self, p):
        for src, dst in self.strips(p, self.whole):
            self.far(src, dst, 0, p, "sib").start()
        for i in PAIR:
            def send(i=i):
                self.far(self.shard_rows(p, i), self.rows(p, i, self.x), 5, 2 * p + i, "sib").start()
            self.mine(p, i, send)

    def pass_on(self, p):
        block = self.block(p, self.xn, self.part(self.y))
        self.far(block, block, 1, p, "xn").wait_recv()
        if self.halves:
            self.far(block, block, 2, p, "yn").start()
        self.far(block, block, 3, p, "sib").start()
        for i in PAIR:
            def send(i=i):
                rows = self.rows(p, i, 1 - self.x, self.half(self.y))
                self.far(rows, rows, 6, 2 * p + i, "xn").wait_recv()
                if self.halves:
                    self.far(rows, rows, 7, 2 * p + i, "yn").start()
                self.far(rows, rows, 8, 2 * p + i, "sib").start()
            self.mine(p, i, send)

    def pass_on_y(self, p):
        block = self.block(p, self.xn, self.part(1 - self.y))
        self.far(block, block, 2, p, "yn").wait_recv()
        self.far(block, block, 4, p, "sib").start()
        for i in PAIR:
            def send(i=i):
                rows = self.rows(p, i, 1 - self.x, 1 - self.y)
                self.far(rows, rows, 7, 2 * p + i, "yn").wait_recv()
                self.far(rows, rows, 9, 2 * p + i, "sib").start()
            self.mine(p, i, send)

    def arrived(self, p):
        block = self.gu.at[p, :, pl.ds(0, 2 * C), :]
        self.far(block, block, 0, p, "sib").wait_recv()
        for i in PAIR:
            def wait(i=i):
                rows = self.wd.at[p, pl.ds(0, STRIP), :]
                self.far(rows, rows, 5, 2 * p + i, "sib").wait_recv()
            pl.when(self.owner(p, i) != self.c)(wait)

    def finish(self):
        for kind in (range(10) if self.halves else (0, 1, 3, 5, 6, 8)):
            all_rows = kind in (0, 5) or not self.halves
            if kind < 5:
                block = self.gu.at[:, :, pl.ds(0, C if all_rows else STRIP), :]
            else:
                block = self.wd.at[:, pl.ds(0, PART), :] if all_rows else self.wd.at[:, pl.ds(0, PART), pl.ds(0, HALF)]
            self.far(block, block, kind, 0, "sib").wait_send()


def kernel(x_hbm, dy_hbm, w_gate, w_up, w_down,
           h_hbm, a0_hbm, gate_hbm, up_hbm, wd0_hbm, gu1_hbm, wd1_hbm, gg_hbm, gu_hbm, gd_hbm, factor_ref,
           a, da, ht, sq, sqs,
           isem, osem, tsem, wsem, xsem, own, gsem0, dsem0, sends0, gsem1, dsem1, sends1, outs_sem, dsem, ra, rb, rc, sa, sb, sc, fsem, inside):
    shards = (w_gate, w_up, w_down)
    g1 = Gather(1, shards, gu1_hbm, wd1_hbm, (gsem1, dsem1), sends1, False)
    me, x, c, peers = g1.me, g1.x, g1.c, g1.peers

    def move(src, dst, sem):
        return pltpu.make_async_copy(src, dst, sem)

    def tile(hbm, j, back=False):
        k = lax.rem(j, 4)
        there, here = hbm.at[ds(j * R, R)], ht.at[k]
        return move(here, there, xsem.at[1, k]) if back else move(there, here, xsem.at[0, k])

    def first_layer(gu, wd, xt, gt, ut, *act):
        g0 = Gather(0, shards, gu, wd, (gsem0, dsem0), sends0, True)

        def saves(p, t, slot):
            return [move(src.at[slot], dst.at[p, ds(t * LONG, LONG)], osem.at[slot, i]) for i, (src, dst) in enumerate(((gt, gate_hbm), (ut, up_hbm)))]

        def local(p, wait):
            if wait:
                block = g0.block(p, me, g0.whole)
                move(block, block, own.at[p, 2]).wait()
            else:
                for src, dst in g0.strips(p, g0.whole):
                    move(src, dst, own.at[p, 2]).start()
            for i in PAIR:
                def go(i=i):
                    copy = move(g0.shard_rows(p, i), g0.rows(p, i, x), own.at[p, i])
                    copy.wait() if wait else copy.start()
                g0.mine(p, i, go)

        def keep(p):
            return move(wd.at[p], wd0_hbm.at[p], fsem.at[3])

        xin = [move(x_hbm.at[pl.ds(t * T, T)], a.at[t], isem.at[0, t]) for t in range(TRIPS)]
        turned = [move(xt.at[odd_], a0_hbm.at[t, :, pl.ds(R * odd_, R)], isem.at[1, 2 * t + odd_]) for t in range(TRIPS) for odd_ in PAIR]
        for copy in xin:
            copy.start()
        barrier = pltpu.get_barrier_semaphore()
        for peer in peers.values():
            pl.semaphore_signal(barrier, inc=1, device_id=peer, device_id_type=MESH)
        pl.semaphore_wait(barrier, len(peers))

        def issue0(p):
            g0.issue(p)

            @pl.when(p < 2)
            def _():
                g0.issue_near(p)
                local(p, False)

        loop(0, 2, issue0)
        for t in range(TRIPS):
            xin[t].wait()

            def put(rows, scale):
                a[t, rows, :] = (up(a[t, rows, :]) * scale).astype(BF)

            passes(T, lambda rows: scale_of(up(a[t, rows, :])), put, 8)
            for h in PAIR:
                if t >= 1:
                    turned[2 * t + h - 2].wait()
                for k in PAIR:
                    xt[h, :, C * k : C * (k + 1)] = a[t, R * h + C * k : R * h + C * (k + 1), :].T
                turned[2 * t + h].start()
            if t == 0:
                loop(2, NC, issue0)
            if t == 1:
                g0.pass_on(0)
            if t == 2:
                g0.pass_on(1)
        g0.pass_on_y(0)

        def down(i, j, p):
            rows = ds(j * R, R)
            da[rows, :] = jnp.where(p == 0, 0.0, da[rows, :]) + dot(act[i][...], wd[jnp.maximum(p, 0)], NN)

        def chunk(p):
            def trip(t):
                now = 2 * p + t

                @pl.when((now >= 1) & (now + 1 < NC))
                def _():
                    g0.pass_on(now + 1)

                @pl.when((now == 1) | (now >= 3) & (now <= NC))
                def _():
                    g0.pass_on_y(jnp.maximum(now - 1, 1))

                @pl.when(now + 2 < NC)
                def _():
                    g0.issue_near(now + 2)
                    local(now + 2, False)

                @pl.when(now < NC)
                def _():
                    g1.issue(now)

                @pl.when(now >= NC)
                def _():
                    g1.issue_near(now - NC)

                @pl.when(now == 2 * NC - 1)
                def _():
                    for j in range(WIDE):
                        tile(x_hbm, j).start()

                early = (2 * (now - AT) + 4) // 5

                @pl.when((now >= AT) & ((5 * early) // 2 == now - AT) & (early < EARLY))
                def _():
                    g1.pass_on(early)

                @pl.when(t == 0)
                def _():
                    local(p, True)
                    g0.arrived(p)
                    keep(p).start()

                @pl.when(now >= 2)
                def _():
                    for copy in saves(0, 0, t):
                        copy.wait()

                for i in range(WIDE):
                    part, j = pl.ds(i * R, R), WIDE * t + i
                    at = a[2 * t + i // 2, i % 2 * R : (i % 2 + 1) * R, :]
                    gt[t, part] = dot(at, gu[p, 0], NN)
                    ut[t, part] = dot(at, gu[p, 1], NN)
                    down(1 - i % 2, *before(j, p, TILES))
                    for k in range(0, R, PB):
                        g, u = gt[t, pl.ds(i * R + k, PB)], ut[t, pl.ds(i * R + k, PB)]
                        act[i % 2][k : k + PB] = (g / (1.0 + jnp.exp(-g)) * u).astype(BF)
                for copy in saves(p, t, t):
                    copy.start()

            loop(0, N // LONG, trip)

        loop(0, NC, chunk)
        down(1, TILES - 1, NC - 1)
        for copy in turned[-2:]:
            copy.wait()
        for o in PAIR:
            for copy in saves(0, 0, o):
                copy.wait()
        move(wd, wd0_hbm, fsem.at[3]).wait()
        g0.finish()

    pl.run_scoped(first_layer, pltpu.VMEM((NC, 2, D, C), BF), pltpu.VMEM((NC, C, D), BF), pltpu.VMEM((2, D, R), BF), *[pltpu.VMEM((2, LONG, C), F32)] * 2, *[pltpu.VMEM((R, C), BF)] * 2)

    def rest(dy, wd, acc_g, acc_u, acc_d, send_a, recv_a, own_b, send_b, recv_b, send_c, recv_c, out_gu, out_d):
        L = 2 * NC - 1

        def copy_a(u, m):
            return pltpu.make_async_remote_copy(send_a.at[m], recv_a.at[odd(u), m], sa, ra.at[odd(u), m], device_id=peers["sib"], device_id_type=MESH)

        def copy_b(u, m):
            s, q = odd(u), lax.rem(u, 4)
            return pltpu.make_async_remote_copy(send_b.at[s, m], recv_b.at[q, m], sb.at[s], rb.at[q, m], device_id=peers["xn"], device_id_type=MESH)

        def copy_c(u, m):
            s, q = odd(u), lax.rem(u, 4)
            return pltpu.make_async_remote_copy(send_c.at[s, m], recv_c.at[q, m], sc.at[s], rc.at[q, m], device_id=peers["yn"], device_id_type=MESH)

        def free(ref, sem, when=True):
            pl.when(when)(lambda: move(ref, ref, sem).wait())

        def outs(u, m):
            s, layer, p = odd(u), 1 - u // NC, lax.rem(u, NC)
            sem = outs_sem.at[s]
            for i in PAIR:
                if m < 2:
                    move(out_gu.at[s, m, :, pl.ds(STRIP * i, STRIP)], (gg_hbm, gu_hbm)[m].at[layer, :, ds((p + NC * i) * STRIP, STRIP)], sem).start()
                    continue
                src = out_d.at[s, pl.ds(PART * i, PART), :]
                dst = gd_hbm.at[layer, ds((2 * p + i - NC * g1.owner(p, i)) * PART, PART), ds(HALF * c, HALF)]
                g1.mine(p, i, lambda: move(src, dst, sem).start(),
                        lambda: pltpu.make_async_remote_copy(src, dst, sem, dsem.at[layer], device_id=peers["sib"], device_id_type=MESH).start())

        def part(s, m, xd, cc):
            if m < 2:
                return [(pl.ds(0, C), (acc_g, acc_u)[m][s, ds(2 * C * xd + C * cc, C), :])]
            return [(pl.ds(STRIP * k, STRIP), acc_d[s, ds(STRIP * xd, STRIP), ds(HALF * cc + C * k, C)]) for k in PAIR]

        def stage_a(u):
            free(send_a, sa, u >= 1)
            for m in THREE:
                for xd in PAIR:
                    for rows, term in part(odd(u), m, xd, 1 - c):
                        send_a[m, xd, rows, :] = term.astype(BF)
                copy_a(u, m).start()

        def stage_b(u):
            s = odd(u)
            free(send_b.at[s], sb.at[s], u >= 2)
            for m in THREE:
                copy_a(u, m).wait_recv()
                for rows, term in part(s, m, 1 - x, c):
                    send_b[s, m, rows, :] = (term + up(recv_a[s, m, 1 - x, rows, :])).astype(BF)
                copy_b(u, m).start()
            for m in THREE:
                for rows, term in part(s, m, x, c):
                    own_b[s, m, rows, :] = term + up(recv_a[s, m, x, rows, :])

        def across(u, matrices):
            s = odd(u)
            for m in matrices:
                copy_b(u, m).wait_recv()
                send_c[s, m] = (own_b[s, m] + up(recv_b[lax.rem(u, 4), m])).astype(BF)
                copy_c(u, m).start()

        def stage_c0(u):
            free(send_c.at[odd(u)], sc.at[odd(u)], u >= 2)
            across(u, THREE[:1])

        def stage_c(u):
            across(u, THREE[1:])

        def stage_d(u):
            s = odd(u)
            free(recv_b.at[0], outs_sem.at[s], u >= 2)
            for m in THREE:
                copy_c(u, m).wait_recv()
                total = (up(send_c[s, m]) + up(recv_c[lax.rem(u, 4), m])).astype(BF)
                if m < 2:
                    out_gu[s, m] = total
                else:
                    for k in PAIR:
                        out_d[s, :, C * k : C * (k + 1)] = total[STRIP * k : STRIP * (k + 1)]
                sq[m] += jnp.sum((up(total) * up(total)).reshape(C // 8, 8, C), axis=0)
                outs(u, m)

        def travel(u, event, when):
            for stage, lag in (((stage_c, 3),), ((stage_a, 1), (stage_d, 4), (stage_c0, 2)), ((stage_b, 1),))[event]:
                @pl.when(when & (u >= lag))
                def _():
                    stage(u - lag)

        def load0(p, slot):
            return move(wd0_hbm.at[p], wd.at[slot], wsem.at[slot, 2])

        def saved(p, t):
            return [move(src.at[p, ds(t * LONG, LONG)], da.at[ds(t * LONG, LONG), pl.ds(C * i, C)], tsem.at[t, i]) for i, src in enumerate((gate_hbm, up_hbm))]

        def dyin(t):
            return move(dy_hbm.at[ds(t * T, T)], dy.at[ds(t * T, T)], isem.at[0, t])

        def new(t):
            return move(a0_hbm.at[t], a.at[t], isem.at[1, t])

        def arithmetic(rows, dt, act, dg, du):
            def pointwise(block, i, gate_and_up):
                for k in range(0, R, PB):
                    (g, u), d, there = gate_and_up(k), up(dt[odd_of(block, i), k : k + PB].astype(BF)), slice(R * i + k, R * i + k + PB)
                    sig = 1.0 / (1.0 + jnp.exp(-g))
                    silu = g * sig
                    act[block][there] = (silu * u).astype(BF)
                    du[block][there] = (d * silu).astype(BF)
                    dg[block][there] = (d * u * (sig + silu * (1.0 - sig))).astype(BF)

            def odd_of(block, i):
                return i if rows == T else block

            def weight_grads(block, k, u, turned=False, row=None):
                s, n = odd(u + 2), k if row is None else row
                dyt = dy[ds(n * rows, rows), :]
                at, how = (a[n], NN) if turned else (a[n // 2, R * block : R * (block + 1), :], TN)
                acc_g[s] = jnp.where(k == 0, 0.0, acc_g[s]) + dot(at, dg[block][...], how)
                acc_u[s] = jnp.where(k == 0, 0.0, acc_u[s]) + dot(at, du[block][...], how)
                acc_d[s] = jnp.where(k == 0, 0.0, acc_d[s]) + dot(act[block][...], dyt, TN)

            return pointwise, weight_grads

        def last_layer(wgu, gt, ut, dt, act0, act1, dg0, dg1, du0, du1):
            dg, du = (dg0, dg1), (du0, du1)
            pointwise, weight_grads = arithmetic(R, dt, (act0, act1), dg, du)

            def loads(p, slot, wait):
                for ref, sem in ((wgu.at[slot], wsem.at[slot, 0]), (wd.at[slot], wsem.at[slot, 1])):
                    if wait:
                        move(ref, ref, sem).wait()
                if wait:
                    return

                def go(src, dst, k):
                    move(src, dst, wsem.at[slot, k]).start()

                for m in PAIR:
                    for k in PAIR:
                        go(shards[m].at[1, :, ds((p + NC * k) * STRIP, STRIP)], wgu.at[slot, m, ds(C * me, C), pl.ds(STRIP * k, STRIP)], 0)
                for owner in (g1.sib, g1.xn, g1.diagonal):
                    go(g1.block(p, owner, g1.whole), wgu.at[slot, :, ds(C * owner, C), :], 0)
                for i in PAIR:
                    there = wd.at[slot, ds(STRIP * x + PART * i, PART), :]
                    g1.mine(p, i, lambda: go(g1.shard_rows(p, i), there, 1), lambda: go(g1.rows(p, i, x), there, 1))
                go(wd1_hbm.at[p, ds(STRIP * (1 - x), STRIP), :], wd.at[slot, ds(STRIP * (1 - x), STRIP), :], 1)

            neighbours = ("sib", "xn", "yn")
            for which in neighbours:
                pl.semaphore_signal(inside, inc=1, device_id=peers[which], device_id_type=MESH)
            g1.arrived(0)
            loads(0, 0, False)
            for t in range(TRIPS):
                dyin(t).start()
            sq[...] = jnp.zeros_like(sq)

            def output(j):
                tile(x_hbm, j).wait()
                k, t, h = lax.rem(j, 4), j // 2, odd(j)

                def sums(rows):
                    value = (up(ht[k, rows, :]) + up(da[ds(j * R + rows.start, ROWS), :].astype(BF))).astype(BF)
                    ht[k, rows, :] = value
                    return scale_of(up(value))

                def put(rows, scale):
                    a[t, ds(h * R + rows.start, ROWS), :] = (up(ht[k, rows, :]) * scale).astype(BF)

                passes(R, sums, put, 16)
                tile(h_hbm, j, True).start()

            def norm_back(j):
                tile(h_hbm, j).wait()
                k = lax.rem(j, 4)

                def parts(part):
                    rows = ds(j * R + part.start, ROWS)
                    return rows, up(ht[k, part, :]), up(da[rows, :].astype(BF))

                def sums(part):
                    _, wide, g = parts(part)
                    scale = scale_of(wide)
                    return scale, jnp.sum(g * wide, -1, keepdims=True) * (scale * scale * scale * (1.0 / D))

                def put(part, value):
                    rows, wide, g = parts(part)
                    scale, inner = value
                    dy[rows, :] = (up(dy[rows, :]) + up((g * scale - wide * inner).astype(BF))).astype(BF)

                passes(R, sums, put, 8)

                @pl.when(odd(j) == 1)
                def _():
                    new(j // 2).start()

                @pl.when(j + 4 < TILES)
                def _():
                    tile(h_hbm, j + 4).start()

            def input_grads(i, j, u, row=None):
                w, rows = odd(u + 2), ds((j if row is None else row) * R, R)
                da[rows, :] = jnp.where(u == 0, 0.0, da[rows, :]) + dot(dg[i][...], wgu[w, 0], NT) + dot(du[i][...], wgu[w, 1], NT)

            def chunk1(u):
                w = odd(u)
                loads(u, w, True)

                @pl.when(u == NC - 1)
                def _():
                    for j in range(4):
                        tile(h_hbm, j).start()

                def trip(t):
                    now = 2 * u + t
                    first, last = u == 0, u == NC - 1
                    travel(u, 0, t == 0)
                    travel(u, 1, t == 1)

                    @pl.when(first)
                    def _():
                        for i in range(WIDE):
                            output(WIDE * t + i)
                        for i in PAIR:
                            dyin(2 * t + i).wait()

                    @pl.when(now == 2)
                    def _():
                        pl.semaphore_wait(inside, len(neighbours))
                        for j in range(TILES - WIDE, TILES):
                            tile(h_hbm, j, True).wait()

                    @pl.when(EARLY + now < NC)
                    def _():
                        g1.pass_on(EARLY + now)

                    @pl.when((t == 1) & (u + 1 < NC))
                    def _():
                        g1.arrived(u + 1)
                        loads(u + 1, 1 - w, False)

                    @pl.when((t == 1) & last)
                    def _():
                        load0(0, 1 - w).start()
                        for j in range(WIDE - 1):
                            norm_back(j)

                    for i in range(WIDE):
                        j, b, part = WIDE * t + i, i % 2, slice(i % 2 * R, (i % 2 + 1) * R)
                        at, dyt = a[2 * t + i // 2, part, :], dy[ds(j * R, R), :]
                        gt[b] = dot(at, wgu[w, 0], NN)
                        ut[b] = dot(at, wgu[w, 1], NN)
                        dt[b] = dot(dyt, wd[w], NT)
                        pj, pu = before(j, u, TILES)
                        row = jnp.where((now == 0) & (i == 0), 1 - b, pj)
                        input_grads(1 - b, pj, pu, row)
                        weight_grads(1 - b, pj, pu, False, row)
                        pointwise(b, 0, lambda k: (gt[b, k : k + PB], ut[b, k : k + PB]))

                    @pl.when(now == 0)
                    def _():
                        for j in range(WIDE):
                            tile(h_hbm, j, True).wait()
                            tile(x_hbm, j + WIDE).start()

                    travel(u, 2, t == 1)

                loop(0, N // LONG, trip)

            loop(0, NC, chunk1)
            input_grads(1, TILES - 1, NC - 1)
            weight_grads(1, TILES - 1, NC - 1)
            norm_back(WIDE - 1)
            for copy in saved(0, 0):
                copy.start()
            for j in range(WIDE, TILES):
                norm_back(j)

        def first_backward(dt, act0, act1, dg0, dg1, du0, du1):
            pointwise, weight_grads = arithmetic(T, dt, (act0, act1), (dg0, dg1), (du0, du1))
            for ref in (act1, dg1, du1):
                ref[...] = jnp.zeros_like(ref)

            def chunk0(u):
                w, p = odd(u), u - NC
                load0(p, w).wait()

                @pl.when(p + 1 < NC)
                def _():
                    load0(p + 1, 1 - w).start()

                def trip(t):
                    travel(u, 0, t == 0)
                    travel(u, 1, t == 1)

                    @pl.when(p == 0)
                    def _():
                        for i in PAIR:
                            new(2 * t + i).wait()

                    for copy in saved(p, t):
                        copy.wait()

                    @pl.when((t == 0) | (p + 1 < NC))
                    def _():
                        for copy in saved(p + t, 1 - t):
                            copy.start()

                    for block in PAIR:
                        k = 2 * t + block
                        for i in PAIR:
                            dt[i] = dot(dy[ds(k * T + i * R, R), :], wd[w], NT)
                            if i == 0:
                                pk, pu = before(k, u, TRIPS)
                                weight_grads(1 - block, pk, pu, True, jnp.where((p == 0) & (k == 0), 0, pk))

                            def gate_and_up(part):
                                rows = ds(k * T + i * R + part, PB)
                                return da[rows, :C], da[rows, C : 2 * C]

                            pointwise(block, i, gate_and_up)

                    travel(u, 2, t == 1)

                loop(0, N // LONG, trip)

            loop(NC, 2 * NC, chunk0)
            stage_c(L - 2)
            weight_grads(1, TRIPS - 1, L, True)

        f, third = pltpu.VMEM, pltpu.VMEM((2, R, C), F32)
        pl.run_scoped(last_layer, f((2, 2, D, C), BF), *[third] * 3, *[f((R, C), BF)] * 6)
        pl.run_scoped(first_backward, third, *[f((T, C), BF)] * 6)

        for stage, u in ((stage_a, L), (stage_d, L - 3), (stage_b, L), (stage_c0, L - 1), (stage_c, L - 1), (stage_d, L - 2), (stage_c0, L), (stage_c, L), (stage_d, L - 1), (stage_d, L)):
            stage(u)
        free(send_a, sa)
        for s in PAIR:
            free(send_b.at[s], sb.at[s])
            free(send_c.at[s], sc.at[s])
        squares = sq[0] + sq[1] + sq[2]
        sqs[me] = squares[:, :STRIP] + squares[:, STRIP:]
        others = [pltpu.make_async_remote_copy(sqs.at[me], sqs.at[me], fsem.at[k], dsem.at[2 + k], device_id=peers[which], device_id_type=MESH)
                  for k, which in enumerate(("sib", "xn", "diagonal"))]
        for copy in others:
            copy.start()
        g1.finish()
        for copy in others:
            copy.wait()
        mean = jnp.sum(sqs[...]) / (3.0 * 2 * D * FF)
        factor = jnp.minimum(1.0, 0.5 * lax.rsqrt(jnp.full((8, STRIP), mean) + 1e-30))
        factor_ref[0, 0] = jnp.max(factor)
        for s in PAIR:
            free(recv_b.at[0], outs_sem.at[s])
        for layer in PAIR:
            got = gd_hbm.at[layer, :, ds(HALF * (1 - c), HALF)]
            move(got, got, dsem.at[layer]).wait()

    piece, f = (3, C, C), pltpu.VMEM
    pl.run_scoped(
        rest,
        f((N, D), BF), f((2, C, D), BF), f((2, D, C), F32), f((2, D, C), F32), f((2, C, D), F32),
        f((3, 2, C, C), BF), f((2, 3, 2, C, C), BF), f((2,) + piece, F32),
        f((2,) + piece, BF), f((4,) + piece, BF), f((2,) + piece, BF), f((4,) + piece, BF), f((2, 2, C, C), BF), f((2, STRIP, HALF), BF),
    )


def gradients(x, dy, *shards):
    dma, shape = pltpu.SemaphoreType.DMA, jax.ShapeDtypeStruct
    sides = [[dma((kinds, NC)), dma((kinds, 2 * NC)), dma((10,))] for kinds in (3, 2)]
    return pl.pallas_call(
        kernel,
        name="gradients",
        in_specs=[ANY] * 5,
        out_specs=[ANY] * 10 + [pl.BlockSpec(memory_space=pltpu.SMEM)],
        out_shape=[shape((N, D), BF), shape((TRIPS, D, T), BF), shape((NC, N, C), F32), shape((NC, N, C), F32),
                   shape((NC, C, D), BF), shape((NC, 2, D, C), BF), shape((NC, C, D), BF),
                   shape((2, C, FF), BF), shape((2, C, FF), BF), shape((2, FF // 4, D), BF), shape((1, 1), F32)],
        scratch_shapes=[
            pltpu.VMEM((TRIPS, T, D), BF), pltpu.VMEM((N, D), F32), pltpu.VMEM((4, R, D), BF),
            pltpu.VMEM((3, 8, C), F32), pltpu.VMEM((4, 8, STRIP), F32),
            dma((2, TILES)), *[dma((2, 2))] * 2, dma((2, 3)), dma((2, 4)), dma((NC, 3)), *sides[0], *sides[1], dma((2,)), dma((5,)),
            dma((2, 3)), dma((4, 3)), dma((4, 3)), dma(()), dma((2,)), dma((2,)), dma((4,)), pltpu.SemaphoreType.REGULAR,
        ],
        compiler_params=pltpu.CompilerParams(vmem_limit_bytes=67_000_000, collective_id=0, has_side_effects=True),
    )(x, dy, *shards)[-4:]


def adamw(w, m, v, g):
    m = 0.9 * m + 0.1 * g
    v = 0.95 * v + 0.05 * g * g
    step = m * lax.rsqrt(v + 1e-8) + 0.1 * w
    return (w - 0.02 * step).astype(BF), m, v


def solution(mesh):
    def step(x, dy, *arrays):
        weights, m, v = (arrays[i : i + 3] for i in (0, 3, 6))
        *grads, factor = gradients(x[0], dy[0], *weights)
        new = [adamw(up(w), m, v, up(g) * factor[0, 0]) for w, m, v, g in zip(weights, m, v, grads, strict=True)]
        return tuple(one[which] for which in THREE for one in new)

    states, cut = P(("rep", "r", "s"), None, None), P(None, "s", None)
    return jax.shard_map(
        step,
        mesh=mesh,
        in_specs=(states, states) + (cut,) * 9,
        out_specs=(P("rep", "s", None),) * 9,
        check_vma=False,
    )
```
